128 devices in a mesh: row: 16 (over y, z), col: 8 (over x, core).
Axes of the slice: x: 4, y: 4, z: 4, core: 2. Of those that a mesh axis runs over, the one named last changes fastest.
Arguments:
- points: float32 [32768, 64], P(('col', 'row')), may hold values from -6 to 6
- feature_scale: float32 [64], replicated, may hold values from 0.1 to 0.5
- test_matrix: bfloat16 [32768, 256], P(('col', 'row')), may hold values from -6 to 6
- targets: float32 [32768], P(('col', 'row')), may hold values from -6 to 6
- ridge: float32 [1], replicated, may hold values from 0.5 to 2
Outputs:
- coefficients: float32 [32768], P(('col', 'row'))
- residual: float32 [32768], P(('col', 'row'))
- sketch: float32 [32768, 256], P(('col', 'row'))
The draws below stay inside these ranges and needn't reach their ends.
All inputs are finite; a program needn't handle non-finite values.
Results may differ from the reference program's by a relative error of at most 0.012.
The reference program's roundings to bfloat16 on the way count: a program that leaves them out, or rounds other values in their place, can miss the bound.
Values may be sent and summed in bfloat16 or wider, within the bound.
No kernel may reach another device: no remote copies, remote signals or barrier semaphores. Data moves between devices by JAX's collectives and lax.ppermute only.
A program may use at most 128 MiB of HBM per device.

```python
import math
import jax
import jax.numpy as jnp
from jax import lax

FEATURES = 64
RANK = 256
ITERS = 2
POINTS = 32768


def level_of(own_key, dims, pieces, least, top_value):
    loudness, own = 1.0, jax.random.fold_in(own_key, 6)
    for position, blocks in pieces:
        steps = jnp.exp(jax.random.uniform(jax.random.fold_in(own, position), (blocks,), jnp.float32, least / len(pieces), top_value / len(pieces)))
        loudness = loudness * jnp.repeat(steps, dims[position] // blocks).reshape([-1 if axis == position else 1 for axis in range(len(dims))])
    return loudness


def centred(stream_key, extent, deviation, reach, pieces=(), kind=jnp.bfloat16):
    entries = deviation * jax.random.normal(stream_key, extent, jnp.float32)
    if pieces:
        entries = entries * level_of(stream_key, extent, pieces, -0.22, 0.18)
    return jnp.clip(entries, -reach, reach).astype(kind)


def setup_inputs(seed: int = 0) -> dict:
    seeds = jax.random.split(jax.random.key(seed), 6)
    points = centred(seeds[0], (POINTS, FEATURES), 1.0, 6.0, ((0, 128),), jnp.float32)
    feature_scale = jnp.clip(jnp.exp(jax.random.uniform(seeds[1], (FEATURES,), jnp.float32, math.log(0.1), math.log(0.5))), 0.1, 0.5)
    test_matrix = centred(seeds[2], (POINTS, RANK), 1.0, 6.0, ((0, 128),))
    targets = centred(seeds[3], (POINTS,), 1.0, 6.0, ((0, 128),), jnp.float32)
    ridge = jnp.clip(jnp.exp(jax.random.uniform(seeds[4], (1,), jnp.float32, math.log(0.5), math.log(2.0))), 0.5, 2.0)
    return dict(points=points, feature_scale=feature_scale, test_matrix=test_matrix, targets=targets, ridge=ridge)


def kernel_block(left, left_norm, right, right_norm):
    cross = lax.dot_general(left.astype(jnp.float32), right.astype(jnp.float32), (((1,), (1,)), ((), ())), precision=lax.Precision.HIGHEST, preferred_element_type=jnp.float32)
    return jnp.exp(-0.5 * (left_norm[:, None] + right_norm[None, :] - 2.0 * cross))

def core_solve(lower, vector):
    middle = lax.linalg.triangular_solve(lower, vector[:, None], left_side=True, lower=True)
    return lax.linalg.triangular_solve(lower, middle, left_side=True, lower=True, transpose_a=True)[:, 0]

def reference(points, feature_scale, test_matrix, targets, ridge):
    ridge_value = ridge[0]
    scaled = points * feature_scale[None, :]
    norms = jnp.sum(scaled * scaled, axis=1)
    block_rows = math.gcd(POINTS, 512)
    blocks = POINTS // block_rows
    scaled_blocks = scaled.reshape(blocks, block_rows, FEATURES)
    norm_blocks = norms.reshape(blocks, block_rows)
    test_wide = test_matrix.astype(jnp.float32)

    def sketch_rows(pair):
        weights = kernel_block(pair[0], pair[1], scaled, norms).astype(jnp.bfloat16)
        weights = lax.optimization_barrier(weights).astype(jnp.float32)
        return jnp.dot(weights.astype(jnp.float32), test_wide.astype(jnp.float32), precision=lax.Precision.HIGHEST, preferred_element_type=jnp.float32)
    sketch = lax.map(sketch_rows, (scaled_blocks, norm_blocks)).reshape(POINTS, RANK)

    def operate(vector):

        def rows_term(pair):
            weights = kernel_block(pair[0], pair[1], scaled, norms)
            return jnp.dot(weights.astype(jnp.float32), vector.astype(jnp.float32), precision=lax.Precision.HIGHEST, preferred_element_type=jnp.float32)
        return lax.map(rows_term, (scaled_blocks, norm_blocks)).reshape(POINTS) + ridge_value * vector
    gram_test = lax.dot_general(test_wide.astype(jnp.float32), sketch.astype(jnp.float32), (((0,), (0,)), ((), ())), precision=lax.Precision.HIGHEST, preferred_element_type=jnp.float32)
    gram_sketch = lax.dot_general(sketch.astype(jnp.float32), sketch.astype(jnp.float32), (((0,), (0,)), ((), ())), precision=lax.Precision.HIGHEST, preferred_element_type=jnp.float32)
    lower = jnp.linalg.cholesky(ridge_value * gram_test + gram_sketch)

    def precondition(resid):
        projected = jnp.dot(resid.astype(jnp.float32), sketch.astype(jnp.float32), precision=lax.Precision.HIGHEST, preferred_element_type=jnp.float32)
        solved = core_solve(lower, projected)
        return (resid - jnp.dot(sketch.astype(jnp.float32), solved.astype(jnp.float32), precision=lax.Precision.HIGHEST, preferred_element_type=jnp.float32)) / ridge_value
    coefficients = jnp.zeros((POINTS,), jnp.float32)
    resid = targets
    precond = precondition(resid)
    descent = jnp.sum(resid * precond)
    direction = precond
    for turn in range(ITERS):
        image = operate(direction)
        step_size = descent / jnp.sum(direction * image)
        coefficients = coefficients + step_size * direction
        if turn + 1 < ITERS:
            resid = resid - step_size * image
            precond = precondition(resid)
            fresh = jnp.sum(resid * precond)
            direction = precond + fresh / descent * direction
            descent = fresh
    residual = targets - operate(coefficients)
    return (coefficients, residual, sketch)
```

```python
import functools

import jax
import jax.numpy as jnp
from jax import lax
from jax.experimental import pallas as pl
from jax.experimental.pallas import tpu as pltpu
from jax.sharding import Mesh
from jax.sharding import PartitionSpec as P

ROW = ("row_0", "row_1")
COL = ("col_0", "col_1")
COL_ROW = ("col_0", "col_1", "row_0", "row_1")
LOG2E = 1.4426950408889634
MIB = 1024 * 1024
F32 = jnp.float32
BF16 = jnp.bfloat16
HIGH = lax.Precision.HIGHEST


def call(body, outs, *args, scratch=(), limit=16, name=None):
    return pl.pallas_call(
        body,
        out_shape=outs,
        scratch_shapes=list(scratch),
        compiler_params=pltpu.CompilerParams(vmem_limit_bytes=limit * MIB),
        name=name,
    )(*args)


def shape(*dims, dtype=F32):
    return jax.ShapeDtypeStruct(dims, dtype)


def exchanged(pieces, axes):
    return lax.all_to_all(pieces, axes, 0, 0, tiled=True)


def from_everyone(value, axes):
    copies = lax.axis_size(axes)
    return exchanged(jnp.broadcast_to(value[None], (copies, *value.shape)), axes)


def split3(value):
    first = value.astype(BF16)
    rest = value - first.astype(F32)
    second = rest.astype(BF16)
    third = (rest - second.astype(F32)).astype(BF16)
    return first, second, third


def features_body(points_ref, scale_ref, out_ref):
    y = points_ref[...] * scale_ref[...]
    rows = y.shape[0]
    norm = -0.5 * jnp.sum(y * y, axis=1, keepdims=True)
    first, second, third = split3(y)
    n1, n2, n3 = (part.astype(F32) for part in split3(norm))
    lane = lax.broadcasted_iota(jnp.int32, (rows, 64), 1)
    zero = jnp.zeros((rows, 64), F32)
    norms = zero
    for at, part in ((0, n1), (1, n2), (2, n3), (3, n1), (4, n2), (5, n3)):
        norms = jnp.where(lane == at, part, norms)
    out_ref[:, :128] = jnp.concatenate([first.astype(F32), second.astype(F32)], axis=1).astype(BF16)
    out_ref[:, 128:] = jnp.concatenate([third.astype(F32), norms], axis=1).astype(BF16)


def kernel_body(left_ref, right_ref, test_ref, kern_ref, sketch_ref, right_scr, *, chunk):
    lane = lax.broadcasted_iota(jnp.int32, (1, 128), 1)

    def mask(test):
        return jnp.where(test, 1.0, 0.0).astype(BF16)

    low = mask(lane < 64)
    left_norm = mask((lane >= 64) & (lane < 67))
    right_norm = mask((lane >= 67) & (lane < 70))

    @pl.when(pl.program_id(0) == 0)
    def _():
        m1 = right_ref[:, :128]
        m2 = right_ref[:, 128:256]
        right_scr[:, 0:128] = m1
        right_scr[:, 128:256] = pltpu.roll(m1.astype(F32), 64, 1).astype(BF16)
        right_scr[:, 256:384] = m2 * (low + right_norm) + left_norm
        right_scr[:, 384:512] = m1 * low

    m1 = left_ref[:, :128]
    m2 = left_ref[:, 128:256]
    left = jnp.concatenate(
        [m1, m1, m1 * low + m2 * left_norm + right_norm, m2 * low], axis=1
    )
    total = None
    for start in range(0, right_ref.shape[0], chunk):
        exponent = lax.dot_general(
            left,
            right_scr[start : start + chunk, :],
            (((1,), (1,)), ((), ())),
            preferred_element_type=F32,
        )
        weights = jnp.exp2(exponent)
        kern_ref[:, start : start + chunk] = weights
        part = jnp.dot(
            weights.astype(BF16), test_ref[start : start + chunk, :], preferred_element_type=F32
        )
        total = part if total is None else total + part
    sketch_ref[...] = total


def kernel_and_sketch(left, right, test, tile=512, chunk=512):
    rows, columns, rank = left.shape[0], right.shape[0], test.shape[1]
    return pl.pallas_call(
        functools.partial(kernel_body, chunk=chunk),
        grid=(rows // tile,),
        in_specs=[
            pl.BlockSpec((tile, 256), lambda i: (i, 0)),
            pl.BlockSpec((columns, 256), lambda i: (0, 0)),
            pl.BlockSpec((columns, rank), lambda i: (0, 0)),
        ],
        out_specs=[
            pl.BlockSpec((tile, columns), lambda i: (i, 0)),
            pl.BlockSpec((tile, rank), lambda i: (i, 0)),
        ],
        out_shape=[shape(rows, columns), shape(rows, rank)],
        scratch_shapes=[pltpu.VMEM((columns, 512), BF16)],
        compiler_params=pltpu.CompilerParams(vmem_limit_bytes=48 * MIB),
        name="kernel_and_sketch",
    )(left, right, test)


def core_body(parts_ref, test_ref, targets_ref, ridge_ref, sketch_ref, out_ref):
    sketch = parts_ref[0]
    for i in range(1, parts_ref.shape[0]):
        sketch = sketch + parts_ref[i]
    sketch_ref[...] = sketch
    shifted = ridge_ref[0, 0] * test_ref[...].astype(F32) + sketch
    core = lax.dot_general(
        shifted, sketch, (((0,), (0,)), ((), ())), precision=HIGH, preferred_element_type=F32
    )
    targets = jnp.broadcast_to(targets_ref[...], (8, 256))
    projected = jnp.dot(targets, sketch, precision=HIGH, preferred_element_type=F32)
    square = jnp.sum(targets[0:1] * targets[0:1], axis=1, keepdims=True)
    row = lax.broadcasted_iota(jnp.int32, (8, 256), 0)
    extra = jnp.where(row == 0, projected, jnp.where(row == 1, square, 0.0))
    out_ref[:, 0:256] = core[0:128]
    out_ref[:, 256:512] = core[128:256]
    out_ref[:, 512:768] = jnp.zeros((128, 256), F32)
    out_ref[0:8, 512:768] = extra


def summed_body(parts_ref, out_ref):
    out_ref[...] = jnp.broadcast_to(jnp.sum(parts_ref[...], axis=0, keepdims=True), out_ref.shape)


def inverted(work_ref):
    size = work_ref.shape[0]
    sub = lax.broadcasted_iota(jnp.int32, (8, 1), 0)
    lanes = lax.broadcasted_iota(jnp.int32, (1, size), 1)
    for half in range(size // 128):
        window = slice(half * 128, half * 128 + 128)

        def panel_step(step, carry, half=half, window=window):
            at = half * 128 + step * 8
            columns = work_ref[:, window]
            panel = work_ref[pl.ds(at, 8), :]
            inner = panel[:, window]
            pick = [jnp.full((8, 128), 0, jnp.int32) + (step * 8 + j) for j in range(8)]
            diag = [jnp.take_along_axis(inner, pick[j], axis=1) for j in range(8)]
            for j in range(8):
                inverse = 1.0 / diag[j][j : j + 1, :]
                panel = jnp.where(lanes == at + j, jnp.where(sub == j, 1.0, 0.0), panel)
                wide = jnp.concatenate([inverse] * (size // 128), axis=1)
                row = panel[j : j + 1, :] * wide
                factor = jnp.concatenate([diag[j]] * (size // 128), axis=1)
                panel = jnp.where(sub == j, row, panel - factor * row)
                for k in range(j + 1, 8):
                    pivot_row = diag[k][j : j + 1, :] * inverse
                    diag[k] = jnp.where(sub == j, pivot_row, diag[k] - diag[j] * pivot_row)
            inside = (lanes >= at) & (lanes < at + 8)
            for group in range(size // 8):
                block = jnp.where(inside, 0.0, work_ref[group * 8 : group * 8 + 8, :])
                rows = columns[group * 8 : group * 8 + 8, :]
                for j in range(8):
                    factor = jnp.take_along_axis(rows, pick[j], axis=1)
                    factor = jnp.concatenate([factor] * (size // 128), axis=1)
                    block = block - factor * panel[j : j + 1, :]
                work_ref[group * 8 : group * 8 + 8, :] = block
            work_ref[pl.ds(at, 8), :] = panel
            return carry

        lax.fori_loop(0, 16, panel_step, 0)


def eight(row):
    return jnp.broadcast_to(row, (8, row.shape[1]))


def row_dot(a, b):
    return jnp.sum(a * b, axis=1, keepdims=True)


def times(vector, matrix, transposed=False):
    dims = (((1,), (1 if transposed else 0,)), ((), ()))
    return lax.dot_general(vector, matrix, dims, precision=HIGH, preferred_element_type=F32)


def first_body(packed_ref, sketch_ref, targets_ref, ridge_ref, inverse_ref, state_ref, send_ref):
    inverse_ref[0:128, :] = packed_ref[:, 0:256]
    inverse_ref[128:256, :] = packed_ref[:, 256:512]
    inverted(inverse_ref)
    projected = packed_ref[0:1, 512:768]
    square = packed_ref[1:2, 512:768]
    solved = times(eight(projected), inverse_ref[...])
    fitted = times(solved, sketch_ref[...], transposed=True)
    ridge = ridge_ref[0, 0]
    direction = (targets_ref[...] - fitted[0:1]) / ridge
    descent = (square - row_dot(projected, solved[0:1])) / ridge
    state_ref[0:1, :] = direction
    state_ref[1:2, :] = projected
    state_ref[2:3, :] = square
    state_ref[3:4, :] = descent
    send_ref[...] = jnp.broadcast_to(direction, send_ref.shape)


def product_body(kern_ref, vector_ref, out_ref):
    rows, columns = kern_ref.shape
    pieces = []
    for at in range(0, columns, 256):
        pieces.append(vector_ref[at // 256 : at // 256 + 1, :])
    vector = jnp.concatenate(pieces, axis=1)
    sub = lax.broadcasted_iota(jnp.int32, (8, 128), 0)
    lane = lax.broadcasted_iota(jnp.int32, (8, 128), 1)
    for base in range(0, rows, 128):
        packed = jnp.zeros((8, 128), F32)
        for group in range(16):
            at = base + group * 8
            block = kern_ref[at : at + 8, :] * vector
            acc = [block[:, k * 128 : k * 128 + 128] for k in range(columns // 128)]
            while len(acc) > 1:
                acc = [a + b for a, b in zip(acc[::2], acc[1::2])]
            column = jnp.sum(acc[0], axis=1, keepdims=True)
            packed = packed + jnp.where(lane == sub + group * 8, column, 0.0)
        out_ref[pl.program_id(0), :, base : base + 128] = eight(
            jnp.sum(packed, axis=0, keepdims=True)
        )


def kernel_times(kern, vector, tile=256):
    rows, columns = kern.shape
    out = pl.pallas_call(
        product_body,
        grid=(rows // tile,),
        in_specs=[
            pl.BlockSpec((tile, columns), lambda i: (i, 0)),
            pl.BlockSpec((columns // 256, 256), lambda i: (0, 0)),
        ],
        out_specs=pl.BlockSpec((rows // tile, 8, tile), lambda i: (0, 0, 0)),
        out_shape=shape(rows // tile, 8, tile),
        compiler_params=pltpu.CompilerParams(vmem_limit_bytes=24 * MIB),
        name="kernel_times",
    )(kern, vector)
    return out


def image_body(parts_ref, state_ref, sketch_ref, targets_ref, ridge_ref, image_ref, send_ref):
    image = jnp.sum(parts_ref[...], axis=0)[0:1] + ridge_ref[0, 0] * state_ref[0:1, :]
    image_ref[...] = eight(image)
    along = times(eight(image), sketch_ref[...])[0:1]
    lane = lax.broadcasted_iota(jnp.int32, (1, 128), 1)
    sums = jnp.where(
        lane == 0,
        row_dot(state_ref[0:1, :], image),
        jnp.where(
            lane == 1, row_dot(image, image), jnp.where(lane == 2, row_dot(targets_ref[...], image), 0.0)
        ),
    )
    send_ref[:, 0:256] = jnp.broadcast_to(along, (send_ref.shape[0], 256))
    send_ref[:, 256:384] = jnp.broadcast_to(sums, (send_ref.shape[0], 128))


def second_body(
    parts_ref, state_ref, image_ref, inverse_ref, sketch_ref, targets_ref, ridge_ref, next_ref, send_ref
):
    sums = jnp.sum(parts_ref[...], axis=0, keepdims=True)
    along = sums[:, 0:256]
    curve, image_square, cross = sums[:, 256:257], sums[:, 257:258], sums[:, 258:259]
    ridge = ridge_ref[0, 0]
    descent = state_ref[3:4, :]
    step = descent / curve
    projected = state_ref[1:2, :] - step * along
    solved = times(eight(projected), inverse_ref[...])
    fitted = times(solved, sketch_ref[...], transposed=True)[0:1]
    resid = targets_ref[...] - step * image_ref[0:1, :]
    square = state_ref[2:3, :] - 2.0 * step * cross + step * step * image_square
    fresh = (square - row_dot(projected, solved[0:1])) / ridge
    direction = (resid - fitted) / ridge + fresh / descent * state_ref[0:1, :]
    next_ref[0:1, :] = direction
    next_ref[1:2, :] = step
    next_ref[2:3, :] = fresh
    send_ref[...] = jnp.broadcast_to(direction, send_ref.shape)


def last_image_body(parts_ref, next_ref, ridge_ref, image_ref, send_ref):
    image = jnp.sum(parts_ref[...], axis=0)[0:1] + ridge_ref[0, 0] * next_ref[0:1, :]
    image_ref[...] = eight(image)
    send_ref[...] = jnp.broadcast_to(row_dot(next_ref[0:1, :], image), send_ref.shape)


def finish_body(
    parts_ref, state_ref, next_ref, image_ref, last_ref, targets_ref, coefficients_ref, residual_ref
):
    curve = jnp.sum(parts_ref[...], axis=0, keepdims=True)[:, 0:1]
    step = next_ref[1:2, :]
    last_step = next_ref[2:3, :] / curve
    coefficients_ref[...] = step * state_ref[0:1, :] + last_step * next_ref[0:1, :]
    residual_ref[...] = targets_ref[...] - step * image_ref[0:1, :] - last_step * last_ref[0:1, :]


def local(points, feature_scale, test_matrix, targets, ridge):
    everyone = lax.axis_size(COL_ROW)
    row_devices = lax.axis_size(ROW)
    own, rank = test_matrix.shape
    ridge = ridge.reshape(1, 1)
    targets = targets.reshape(1, own)
    scale = (feature_scale * LOG2E**0.5).reshape(1, -1)
    features = call(
        features_body, shape(own, 256, dtype=BF16), points, scale, name="features"
    )
    left = from_everyone(features, COL).reshape(-1, 256)
    right = from_everyone(features, ROW).reshape(-1, 256)
    test = from_everyone(test_matrix, ROW).reshape(-1, rank)
    kern, sketch_parts = kernel_and_sketch(left, right, test)
    sketch_parts = exchanged(sketch_parts.reshape(-1, own, rank), COL)
    sketch, packed = call(
        core_body,
        [shape(own, rank), shape(everyone, 768)],
        sketch_parts,
        test_matrix,
        targets,
        ridge,
        name="core",
    )
    packed = exchanged(packed, COL_ROW)
    packed = call(summed_body, shape(everyone, 768), packed, name="summed")
    packed = exchanged(packed, COL_ROW)
    inverse, state, send = call(
        first_body,
        [shape(rank, rank), shape(8, own), shape(row_devices, own)],
        packed,
        sketch,
        targets,
        ridge,
        name="first",
    )
    product = kernel_times(kern, exchanged(send, ROW))
    image, send = call(
        image_body,
        [shape(8, own), shape(everyone, 384)],
        exchanged(product, COL),
        state,
        sketch,
        targets,
        ridge,
        name="image",
    )
    following, send = call(
        second_body,
        [shape(8, own), shape(row_devices, own)],
        exchanged(send, COL_ROW),
        state,
        image,
        inverse,
        sketch,
        targets,
        ridge,
        name="second",
    )
    product = kernel_times(kern, exchanged(send, ROW))
    last, send = call(
        last_image_body,
        [shape(8, own), shape(everyone, 128)],
        exchanged(product, COL),
        following,
        ridge,
        name="last_image",
    )
    coefficients, residual = call(
        finish_body,
        [shape(1, own), shape(1, own)],
        exchanged(send, COL_ROW),
        state,
        following,
        image,
        last,
        targets,
        name="finish",
    )
    return coefficients.reshape(own), residual.reshape(own), sketch


def solution(mesh):
    split = Mesh(mesh.devices.reshape(4, 4, 4, 2), ROW + COL)
    return jax.shard_map(
        local,
        mesh=split,
        in_specs=(P(COL_ROW, None), P(), P(COL_ROW, None), P(COL_ROW), P()),
        out_specs=(P(COL_ROW), P(COL_ROW), P(COL_ROW, None)),
        check_vma=False,
    )
```

```python
import functools

import jax
import jax.numpy as jnp
from jax import lax
from jax.experimental import pallas as pl
from jax.experimental.pallas import tpu as pltpu
from jax.sharding import Mesh
from jax.sharding import PartitionSpec as P

ROW = ("row_0", "row_1")
COL = ("col_0", "col_1")
COL_ROW = ("col_0", "col_1", "row_0", "row_1")
LOG2E = 1.4426950408889634
MIB = 1024 * 1024
F32 = jnp.float32
BF16 = jnp.bfloat16
HIGH = lax.Precision.HIGHEST
KERN_SPACE = pltpu.VMEM
KLIMIT = 16
KLIMIT2 = 8


def call(body, outs, *args, scratch=(), limit=16, name=None):
    return pl.pallas_call(
        body,
        out_shape=outs,
        scratch_shapes=list(scratch),
        compiler_params=pltpu.CompilerParams(vmem_limit_bytes=limit * MIB),
        name=name,
    )(*args)


def shape(*dims, dtype=F32):
    return jax.ShapeDtypeStruct(dims, dtype)


def exchanged(pieces, axes):
    return lax.all_to_all(pieces, axes, 0, 0, tiled=True)


def from_everyone(value, axes):
    copies = lax.axis_size(axes)
    return exchanged(jnp.broadcast_to(value[None], (copies, *value.shape)), axes)


def parts_body(points_ref, scale_ref, out_ref):
    y = points_ref[...] * scale_ref[...]
    first = y.astype(BF16).astype(F32)
    second = (y - first).astype(BF16).astype(F32)
    out_ref[...] = jnp.concatenate([first, second], axis=1).astype(BF16)


def doubled(parts):
    wide = parts.astype(F32)
    return wide + pltpu.roll(wide, 64, 1)


def columns_body(message_ref, right_ref, norm_ref, test_ref):
    parts = message_ref[:, 0:128]
    right_ref[:, 0:128] = parts
    right_ref[:, 128:256] = pltpu.roll(parts.astype(F32), 64, 1).astype(BF16)
    test_ref[...] = message_ref[:, 128:384]
    points = doubled(parts)
    norm_ref[...] = times(jnp.full((8, 128), -0.25, F32), points * points, transposed=True)


def block_body(left_ref, right_ref, norm_ref, test_ref, kern_ref, own_ref, other_ref, *, chunk):
    parts = left_ref[...]
    points = doubled(parts)
    left_norm = -0.25 * jnp.sum(points * points, axis=1, keepdims=True)
    left = jnp.concatenate([parts, parts], axis=1)
    total = None
    for start in range(0, right_ref.shape[0], chunk):
        span = slice(start, start + chunk)
        exponent = lax.dot_general(
            left, right_ref[span, :], (((1,), (1,)), ((), ())), preferred_element_type=F32
        )
        weights = jnp.exp2(exponent + left_norm + norm_ref[0:1, span])
        kern_ref[:, span] = weights
        part = jnp.dot(weights.astype(BF16), test_ref[span, :], preferred_element_type=F32)
        total = part if total is None else total + part
    half = total.shape[0] // 2
    own_ref[...] = total[:half]
    other_ref[...] = total[half:]


def kernel_block(left, right, norm, test):
    rows, columns, rank = left.shape[0], right.shape[0], test.shape[1]
    return call(
        functools.partial(block_body, chunk=512),
        [KERN_SPACE((rows, columns), F32), shape(rows // 2, rank), shape(rows // 2, rank)],
        left,
        right,
        norm,
        test,
        limit=KLIMIT,
        name="kernel_block",
    )


def core_body(
    near_ref, swapped_ref, one_ref, two_ref, three_ref, test_ref, targets_ref, ridge_ref, sketch_ref, out_ref
):
    sketch = near_ref[...] + swapped_ref[...] + one_ref[...] + two_ref[...] + three_ref[...]
    sketch_ref[...] = sketch
    shifted = ridge_ref[0, 0] * test_ref[...].astype(F32) + sketch
    core = lax.dot_general(
        shifted, sketch, (((0,), (0,)), ((), ())), precision=HIGH, preferred_element_type=F32
    )
    targets = jnp.broadcast_to(targets_ref[...], (8, 256))
    projected = jnp.dot(targets, sketch, precision=HIGH, preferred_element_type=F32)
    square = jnp.sum(targets[0:1] * targets[0:1], axis=1, keepdims=True)
    row = lax.broadcasted_iota(jnp.int32, (8, 256), 0)
    extra = jnp.where(row == 0, projected, jnp.where(row == 1, square, 0.0))
    out_ref[:, 0:256] = core[0:128]
    out_ref[:, 256:512] = core[128:256]
    out_ref[:, 512:768] = jnp.zeros((128, 256), F32)
    out_ref[0:8, 512:768] = extra


def summed_body(parts_ref, out_ref):
    out_ref[...] = jnp.broadcast_to(jnp.sum(parts_ref[...], axis=0, keepdims=True), out_ref.shape)


def inverted(work_ref, factors_ref):
    size = work_ref.shape[0]
    panels = size // 8
    sub = lax.broadcasted_iota(jnp.int32, (8, 1), 0)
    lanes = lax.broadcasted_iota(jnp.int32, (1, size), 1)

    def column(block, step, j):
        index = jnp.full((8, 128), 0, jnp.int32) + ((step % 16) * 8 + j)
        window = jnp.where(step < 16, block[:, 0:128], block[:, 128:256])
        return jnp.take_along_axis(window, index, axis=1)

    def wide(value):
        return jnp.concatenate([value, value], axis=1)

    def eliminated(panel, step):
        diag = [column(panel, step, j) for j in range(8)]
        for j in range(8):
            inverse = 1.0 / diag[j][j : j + 1, :]
            for k in range(j + 1, 8):
                pivot = diag[k][j : j + 1, :] * inverse
                diag[k] = jnp.where(sub == j, pivot, diag[k] - diag[j] * pivot)
            panel = jnp.where(lanes == step * 8 + j, jnp.where(sub == j, 1.0, 0.0), panel)
            row = panel[j : j + 1, :] * wide(inverse)
            panel = jnp.where(sub == j, row, panel - wide(diag[j]) * row)
        return panel

    def updated(block, factors, panel, step):
        inside = (lanes >= step * 8) & (lanes < step * 8 + 8)
        block = jnp.where(inside, 0.0, block)
        for j in range(8):
            block = block - wide(factors[j]) * panel[j : j + 1, :]
        return block

    for group in range(panels):
        rows = slice(group * 8, group * 8 + 8)
        for j in range(8):
            factors_ref[j, rows, :] = column(work_ref[rows, :], 0, j)

    def panel_step(step, panel):
        at = pl.multiple_of(step * 8, 8)
        following = jnp.minimum(step + 1, panels - 1)
        ahead = pl.ds(pl.multiple_of(following * 8, 8), 8)
        next_panel = updated(
            work_ref[ahead, :], [factors_ref[j, ahead, :] for j in range(8)], panel, step
        )
        next_panel = eliminated(next_panel, following)
        for group in range(panels):
            rows = slice(group * 8, group * 8 + 8)
            block = updated(
                work_ref[rows, :], [factors_ref[j, rows, :] for j in range(8)], panel, step
            )
            work_ref[rows, :] = block
            for j in range(8):
                factors_ref[j, rows, :] = column(block, following, j)
        here = pl.ds(at, 8)
        work_ref[here, :] = panel
        for j in range(8):
            factors_ref[j, here, :] = column(panel, following, j)
        return next_panel

    lax.fori_loop(0, panels, panel_step, eliminated(work_ref[0:8, :], 0))


def eight(row):
    return jnp.broadcast_to(row, (8, row.shape[1]))


def row_dot(a, b):
    return jnp.sum(a * b, axis=1, keepdims=True)


def times(vector, matrix, transposed=False):
    dims = (((1,), (1 if transposed else 0,)), ((), ()))
    return lax.dot_general(vector, matrix, dims, precision=HIGH, preferred_element_type=F32)


def first_body(packed_ref, sketch_ref, targets_ref, ridge_ref, inverse_ref, state_ref, send_ref, factors_ref):
    inverse_ref[0:128, :] = packed_ref[:, 0:256]
    inverse_ref[128:256, :] = packed_ref[:, 256:512]
    inverted(inverse_ref, factors_ref)
    projected = packed_ref[0:1, 512:768]
    square = packed_ref[1:2, 512:768]
    solved = times(eight(projected), inverse_ref[...])
    fitted = times(solved, sketch_ref[...], transposed=True)
    ridge = ridge_ref[0, 0]
    direction = (targets_ref[...] - fitted[0:1]) / ridge
    descent = (square - row_dot(projected, solved[0:1])) / ridge
    state_ref[0:1, :] = direction
    state_ref[1:2, :] = projected
    state_ref[2:3, :] = square
    state_ref[3:4, :] = descent
    send_ref[...] = jnp.broadcast_to(direction, send_ref.shape)


def product_body(place_ref, *refs):
    *kern_refs, vector_ref, out_ref = refs
    columns = kern_refs[0].shape[1]
    vector = jnp.concatenate(
        [vector_ref[i : i + 1, :] for i in range(vector_ref.shape[0])], axis=1
    )
    sub = lax.broadcasted_iota(jnp.int32, (8, 128), 0)
    lane = lax.broadcasted_iota(jnp.int32, (8, 128), 1)
    for number, kern_ref in enumerate(kern_refs):
        for base in range(0, kern_ref.shape[0], 128):

            def group_step(group, packed, kern_ref=kern_ref, base=base):
                block = kern_ref[pl.ds(pl.multiple_of(base + group * 8, 8), 8), :] * vector
                acc = [block[:, k * 128 : k * 128 + 128] for k in range(columns // 128)]
                while len(acc) > 1:
                    acc = [a + b for a, b in zip(acc[::2], acc[1::2])]
                total = jnp.sum(acc[0], axis=1, keepdims=True)
                return packed + jnp.where(lane == sub + group * 8, total, 0.0)

            packed = lax.fori_loop(0, 16, group_step, jnp.zeros((8, 128), F32), unroll=4)
            place = place_ref[2 * number + base // 256]
            out_ref[place, :, base % 256 : base % 256 + 128] = eight(
                jnp.sum(packed, axis=0, keepdims=True)
            )


def kernel_times(place, kerns, vector):
    vmem = pl.BlockSpec(memory_space=pltpu.VMEM)
    return pl.pallas_call(
        product_body,
        in_specs=[pl.BlockSpec(memory_space=pltpu.SMEM)] + [vmem] * (len(kerns) + 1),
        out_specs=vmem,
        out_shape=shape(8, 8, 256),
        compiler_params=pltpu.CompilerParams(vmem_limit_bytes=KLIMIT2 * MIB),
        name="kernel_times",
    )(place, *kerns, vector)


def image_body(parts_ref, state_ref, sketch_ref, targets_ref, ridge_ref, image_ref, send_ref):
    image = jnp.sum(parts_ref[...], axis=0)[0:1] + ridge_ref[0, 0] * state_ref[0:1, :]
    image_ref[...] = eight(image)
    along = times(eight(image), sketch_ref[...])[0:1]
    lane = lax.broadcasted_iota(jnp.int32, (1, 128), 1)
    sums = jnp.where(
        lane == 0,
        row_dot(state_ref[0:1, :], image),
        jnp.where(
            lane == 1, row_dot(image, image), jnp.where(lane == 2, row_dot(targets_ref[...], image), 0.0)
        ),
    )
    send_ref[:, 0:256] = jnp.broadcast_to(along, (send_ref.shape[0], 256))
    send_ref[:, 256:384] = jnp.broadcast_to(sums, (send_ref.shape[0], 128))


def second_body(
    parts_ref, state_ref, image_ref, inverse_ref, sketch_ref, targets_ref, ridge_ref, next_ref, send_ref
):
    sums = jnp.sum(parts_ref[...], axis=0, keepdims=True)
    along = sums[:, 0:256]
    curve, image_square, cross = sums[:, 256:257], sums[:, 257:258], sums[:, 258:259]
    ridge = ridge_ref[0, 0]
    descent = state_ref[3:4, :]
    step = descent / curve
    projected = state_ref[1:2, :] - step * along
    solved = times(eight(projected), inverse_ref[...])
    fitted = times(solved, sketch_ref[...], transposed=True)[0:1]
    resid = targets_ref[...] - step * image_ref[0:1, :]
    square = state_ref[2:3, :] - 2.0 * step * cross + step * step * image_square
    fresh = (square - row_dot(projected, solved[0:1])) / ridge
    direction = (resid - fitted) / ridge + fresh / descent * state_ref[0:1, :]
    next_ref[0:1, :] = direction
    next_ref[1:2, :] = step
    next_ref[2:3, :] = fresh
    send_ref[...] = jnp.broadcast_to(direction, send_ref.shape)


def last_image_body(parts_ref, next_ref, ridge_ref, image_ref, send_ref):
    image = jnp.sum(parts_ref[...], axis=0)[0:1] + ridge_ref[0, 0] * next_ref[0:1, :]
    image_ref[...] = eight(image)
    send_ref[...] = jnp.broadcast_to(row_dot(next_ref[0:1, :], image), send_ref.shape)


def finish_body(
    parts_ref, state_ref, next_ref, image_ref, last_ref, targets_ref, coefficients_ref, residual_ref
):
    curve = jnp.sum(parts_ref[...], axis=0, keepdims=True)[:, 0:1]
    step = next_ref[1:2, :]
    last_step = next_ref[2:3, :] / curve
    coefficients_ref[...] = step * state_ref[0:1, :] + last_step * next_ref[0:1, :]
    residual_ref[...] = targets_ref[...] - step * image_ref[0:1, :] - last_step * last_ref[0:1, :]


def local(points, feature_scale, test_matrix, targets, ridge):
    everyone = lax.axis_size(COL_ROW)
    row_devices = lax.axis_size(ROW)
    own, rank = test_matrix.shape
    ridge = ridge.reshape(1, 1)
    targets = targets.reshape(1, own)
    scale = (feature_scale * LOG2E**0.5).reshape(1, -1)
    parts = call(parts_body, shape(own, 128, dtype=BF16), points, scale, name="parts")
    chips, cores = lax.axis_size("col_0"), lax.axis_size("col_1")
    chunks = {}
    for shift in range(chips):
        for flip in range(cores):
            pairs = [
                (c, (c // 2 + shift) % chips * 2 + (c % 2 ^ flip)) for c in range(chips * cores)
            ]
            chunks[shift, flip] = lax.ppermute(parts, COL, pairs) if shift or flip else parts
    message = jnp.concatenate([parts, test_matrix], axis=1)
    message = from_everyone(message, ROW).reshape(-1, 128 + rank)
    columns = message.shape[0]
    right, norm, test = call(
        columns_body,
        [shape(columns, 256, dtype=BF16), shape(8, columns), shape(columns, rank, dtype=BF16)],
        message,
        name="columns",
    )
    kerns, sums, own_sums = [], [], None
    order = (2, 1, 3, 0)
    for shift in order:
        left = jnp.concatenate([chunks[shift, 0], chunks[shift, 1]], axis=0)
        kern, near, other = kernel_block(left, right, norm, test)
        kerns.append(kern)
        swapped = lax.ppermute(other, "col_1", [(0, 1), (1, 0)])
        if shift:
            pairs = [(c, (c - shift) % chips) for c in range(chips)]
            sums.append(lax.ppermute(near + swapped, "col_0", pairs))
        else:
            sums = [near, swapped] + sums
    chip, core = lax.axis_index("col_0"), lax.axis_index("col_1")
    place = jnp.stack(
        [(chip - shift) % chips * 2 + (core ^ flip) for shift in order for flip in (0, 1)]
    ).astype(jnp.int32)
    sketch, packed = call(
        core_body,
        [shape(own, rank), shape(everyone, 768)],
        *sums,
        test_matrix,
        targets,
        ridge,
        name="core",
    )
    packed = exchanged(packed, COL_ROW)
    packed = call(summed_body, shape(everyone, 768), packed, name="summed")
    packed = exchanged(packed, COL_ROW)
    inverse, state, send = call(
        first_body,
        [shape(rank, rank), shape(8, own), shape(row_devices, own)],
        packed,
        sketch,
        targets,
        ridge,
        scratch=[pltpu.VMEM((8, rank, 128), F32)],
        name="first",
    )
    product = kernel_times(place, kerns, exchanged(send, ROW))
    image, send = call(
        image_body,
        [shape(8, own), shape(everyone, 384)],
        exchanged(product, COL),
        state,
        sketch,
        targets,
        ridge,
        name="image",
    )
    following, send = call(
        second_body,
        [shape(8, own), shape(row_devices, own)],
        exchanged(send, COL_ROW),
        state,
        image,
        inverse,
        sketch,
        targets,
        ridge,
        name="second",
    )
    product = kernel_times(place, kerns, exchanged(send, ROW))
    last, send = call(
        last_image_body,
        [shape(8, own), shape(everyone, 128)],
        exchanged(product, COL),
        following,
        ridge,
        name="last_image",
    )
    coefficients, residual = call(
        finish_body,
        [shape(1, own), shape(1, own)],
        exchanged(send, COL_ROW),
        state,
        following,
        image,
        last,
        targets,
        name="finish",
    )
    return coefficients.reshape(own), residual.reshape(own), sketch


def solution(mesh):
    split = Mesh(mesh.devices.reshape(4, 4, 4, 2), ROW + COL)
    return jax.shard_map(
        local,
        mesh=split,
        in_specs=(P(COL_ROW, None), P(), P(COL_ROW, None), P(COL_ROW), P()),
        out_specs=(P(COL_ROW), P(COL_ROW), P(COL_ROW, None)),
        check_vma=False,
    )
```

```python
import functools

import jax
import jax.numpy as jnp
from jax import lax
from jax.experimental import pallas as pl
from jax.experimental.pallas import tpu as pltpu
from jax.sharding import Mesh
from jax.sharding import PartitionSpec as P

ROW = ("row_0", "row_1")
COL = ("col_0", "col_1")
COL_ROW = ("col_0", "col_1", "row_0", "row_1")
LOG2E = 1.4426950408889634
MIB = 1024 * 1024
F32 = jnp.float32
BF16 = jnp.bfloat16
HIGH = lax.Precision.HIGHEST
KERN_SPACE = pltpu.VMEM
ORDER = (2, 1, 3, 0)
KLIMIT = 4
KLIMIT2 = 4


def call(body, outs, *args, scratch=(), limit=4, name=None):
    return pl.pallas_call(
        body,
        out_shape=outs,
        scratch_shapes=list(scratch),
        compiler_params=pltpu.CompilerParams(vmem_limit_bytes=limit * MIB),
        name=name,
    )(*args)


def shape(*dims, dtype=F32):
    return jax.ShapeDtypeStruct(dims, dtype)


def exchanged(pieces, axes):
    return lax.all_to_all(pieces, axes, 0, 0, tiled=True)


def split3(value):
    first = value.astype(BF16)
    rest = value - first.astype(F32)
    second = rest.astype(BF16)
    third = (rest - second.astype(F32)).astype(BF16)
    return first, second, third


def parts_body(points_ref, scale_ref, test_ref, out_ref, copies_ref):
    y = points_ref[...] * (scale_ref[...] * LOG2E**0.5)
    first = y.astype(BF16).astype(F32)
    second = (y - first).astype(BF16).astype(F32)
    parts = jnp.concatenate([first, second], axis=1).astype(BF16)
    out_ref[...] = parts
    for i in range(copies_ref.shape[0]):
        copies_ref[i, :, 0:128] = parts
        copies_ref[i, :, 128:384] = test_ref[...]


def doubled(parts):
    wide = parts.astype(F32)
    return wide + pltpu.roll(wide, 64, 1)


def columns_body(message_ref, right_ref, norm_ref, test_ref):
    parts = message_ref[:, 0:128]
    right_ref[:, 0:128] = parts
    right_ref[:, 128:256] = pltpu.roll(parts.astype(F32), 64, 1).astype(BF16)
    test_ref[...] = message_ref[:, 128:384]
    points = doubled(parts)
    norm_ref[...] = times(jnp.full((8, 128), -0.25, F32), points * points, transposed=True)


def block_body(left_ref, right_ref, norm_ref, test_ref, kern_ref, own_ref, other_ref, *, chunk):
    parts = left_ref[...]
    points = doubled(parts)
    left_norm = -0.25 * jnp.sum(points * points, axis=1, keepdims=True)
    left = jnp.concatenate([parts, parts], axis=1)
    total = None
    for start in range(0, right_ref.shape[0], chunk):
        span = slice(start, start + chunk)
        exponent = lax.dot_general(
            left, right_ref[span, :], (((1,), (1,)), ((), ())), preferred_element_type=F32
        )
        weights = jnp.exp2(exponent + left_norm + norm_ref[0:1, span])
        kern_ref[:, span] = weights
        part = jnp.dot(weights.astype(BF16), test_ref[span, :], preferred_element_type=F32)
        total = part if total is None else total + part
    half = total.shape[0] // 2
    own_ref[...] = total[:half]
    other_ref[...] = total[half:]


def kernel_block(left, right, norm, test):
    rows, columns, rank = left.shape[0], right.shape[0], test.shape[1]
    return call(
        functools.partial(block_body, chunk=512),
        [KERN_SPACE((rows, columns), F32), shape(rows // 2, rank), shape(rows // 2, rank)],
        left,
        right,
        norm,
        test,
        limit=KLIMIT,
        name="kernel_block",
    )


def core_body(
    near_ref, swapped_ref, one_ref, two_ref, three_ref, test_ref, targets_ref, ridge_ref, sketch_ref, out_ref
):
    sketch = near_ref[...] + swapped_ref[...] + one_ref[...] + two_ref[...] + three_ref[...]
    sketch_ref[...] = sketch
    shifted = ridge_ref[0, 0] * test_ref[...].astype(F32) + sketch
    core = lax.dot_general(
        shifted, sketch, (((0,), (0,)), ((), ())), precision=HIGH, preferred_element_type=F32
    )
    targets = jnp.broadcast_to(targets_ref[...], (8, 256))
    projected = jnp.dot(targets, sketch, precision=HIGH, preferred_element_type=F32)
    square = jnp.sum(targets[0:1] * targets[0:1], axis=1, keepdims=True)
    row = lax.broadcasted_iota(jnp.int32, (8, 128), 0)
    extra = jnp.where(row == 2, square, 0.0)
    extra = jnp.where(row == 1, projected[:, 128:256], extra)
    extra = jnp.where(row == 0, projected[:, 0:128], extra)
    out_ref[:, 0:256] = core[0:128]
    out_ref[:, 256:384] = core[128:256, 128:256]
    out_ref[:, 384:512] = jnp.zeros((128, 128), F32)
    out_ref[0:8, 384:512] = extra


def summed_body(parts_ref, out_ref):
    out_ref[...] = jnp.broadcast_to(jnp.sum(parts_ref[...], axis=0, keepdims=True), out_ref.shape)


def inverted(work_ref):
    size = work_ref.shape[0]
    panels = size // 8
    sub = lax.broadcasted_iota(jnp.int32, (8, 1), 0)
    lanes = lax.broadcasted_iota(jnp.int32, (1, size), 1)

    def column(block, step, j):
        index = jnp.full((8, 128), 0, jnp.int32) + ((step % 16) * 8 + j)
        window = jnp.where(step < 16, block[:, 0:128], block[:, 128:256])
        return jnp.take_along_axis(window, index, axis=1)

    def wide(value):
        return jnp.concatenate([value, value], axis=1)

    def eliminated(panel, step):
        diag = [column(panel, step, j) for j in range(8)]
        for j in range(8):
            inverse = 1.0 / diag[j][j : j + 1, :]
            for k in range(j + 1, 8):
                pivot = diag[k][j : j + 1, :] * inverse
                diag[k] = jnp.where(sub == j, pivot, diag[k] - diag[j] * pivot)
            panel = jnp.where(lanes == step * 8 + j, jnp.where(sub == j, 1.0, 0.0), panel)
            row = panel[j : j + 1, :] * wide(inverse)
            panel = jnp.where(sub == j, row, panel - wide(diag[j]) * row)
        return panel

    def split(value):
        return [part.astype(F32) for part in split3(value)]

    def stacked(parts):
        return jnp.concatenate(parts, axis=0).astype(BF16)

    def panel_step(step, carry):
        panel, factors = carry
        following = jnp.minimum(step + 1, panels - 1)
        here = pl.ds(pl.multiple_of(step * 8, 8), 8)
        ahead = work_ref[pl.ds(pl.multiple_of(following * 8, 8), 8), :]
        inside = (lanes >= step * 8) & (lanes < step * 8 + 8)
        following_rows = jnp.where(inside, 0.0, ahead)
        for j in range(8):
            following_rows = following_rows - wide(column(ahead, step, j)) * panel[j : j + 1, :]
        f1, f2, f3 = split(factors)
        p1, p2, p3 = split(panel)
        update = lax.dot_general(
            stacked([f1, f1, f2, f2, f1, f3]),
            stacked([p1, p2, p1, p2, p3, p1]),
            (((0,), (0,)), ((), ())),
            preferred_element_type=F32,
        )
        work_ref[...] = jnp.where(inside, 0.0, work_ref[...]) - update
        work_ref[here, :] = panel
        following_factors = jnp.where(lanes < following * 8, -following_rows, following_rows)
        return eliminated(following_rows, following), following_factors

    start = work_ref[0:8, :]
    lax.fori_loop(0, panels, panel_step, (eliminated(start, 0), start))


def eight(row):
    return jnp.broadcast_to(row, (8, row.shape[1]))


def row_dot(a, b):
    return jnp.sum(a * b, axis=1, keepdims=True)


def times(vector, matrix, transposed=False):
    dims = (((1,), (1 if transposed else 0,)), ((), ()))
    return lax.dot_general(vector, matrix, dims, precision=HIGH, preferred_element_type=F32)


def first_body(packed_ref, sketch_ref, targets_ref, ridge_ref, inverse_ref, state_ref, send_ref):
    inverse_ref[0:128, :] = packed_ref[:, 0:256]
    inverse_ref[128:256, 0:128] = packed_ref[:, 128:256].T
    inverse_ref[128:256, 128:256] = packed_ref[:, 256:384]
    inverted(inverse_ref)
    projected = jnp.concatenate([packed_ref[0:1, 384:512], packed_ref[1:2, 384:512]], axis=1)
    square = packed_ref[2:3, 384:385]
    solved = times(eight(projected), inverse_ref[...])
    fitted = times(solved, sketch_ref[...], transposed=True)
    ridge = ridge_ref[0, 0]
    direction = (targets_ref[...] - fitted[0:1]) / ridge
    descent = (square - row_dot(projected, solved[0:1])) / ridge
    state_ref[0:1, :] = direction
    state_ref[1:2, :] = projected
    state_ref[2:3, :] = jnp.broadcast_to(square, (1, 256))
    state_ref[3:4, :] = jnp.broadcast_to(descent, (1, 256))
    send_ref[...] = jnp.broadcast_to(direction, send_ref.shape)


def product_body(*refs):
    *kern_refs, vector_ref, out_ref = refs
    tiles = kern_refs[0].shape[1] // 128
    sub = lax.broadcasted_iota(jnp.int32, (8, 128), 0)
    lane = lax.broadcasted_iota(jnp.int32, (8, 128), 1)
    chip, core = lax.axis_index("col_0"), lax.axis_index("col_1")
    chips = len(kern_refs)
    for shift, kern_ref in zip(ORDER, kern_refs):
        for flip in range(2):
            place = (chip + (chips - shift)) % chips * 2 + (core + flip) % 2
            for half in range(2):
                packed = jnp.zeros((8, 128), F32)
                for start in range(0, 128, 64):
                    base = flip * 256 + half * 128 + start
                    acc = [None] * 8
                    for k in range(tiles):
                        piece = eight(
                            vector_ref[k // 2 : k // 2 + 1, k % 2 * 128 : k % 2 * 128 + 128]
                        )
                        for g in range(8):
                            block = kern_ref[
                                base + g * 8 : base + g * 8 + 8, k * 128 : k * 128 + 128
                            ]
                            acc[g] = block * piece if k == 0 else acc[g] + block * piece
                    for g in range(8):
                        total = jnp.sum(acc[g], axis=1, keepdims=True)
                        packed = packed + jnp.where(lane == sub + (start + g * 8), total, 0.0)
                out_ref[place, :, half * 128 : half * 128 + 128] = eight(
                    jnp.sum(packed, axis=0, keepdims=True)
                )


def kernel_times(kerns, vector):
    return call(product_body, shape(8, 8, 256), *kerns, vector, limit=KLIMIT2, name="kernel_times")


def image_body(parts_ref, state_ref, sketch_ref, targets_ref, ridge_ref, image_ref, send_ref):
    image = jnp.sum(parts_ref[...], axis=0)[0:1] + ridge_ref[0, 0] * state_ref[0:1, :]
    image_ref[...] = eight(image)
    along = times(eight(image), sketch_ref[...])[0:1]
    lane = lax.broadcasted_iota(jnp.int32, (1, 128), 1)
    sums = jnp.where(
        lane == 0,
        row_dot(state_ref[0:1, :], image),
        jnp.where(
            lane == 1, row_dot(image, image), jnp.where(lane == 2, row_dot(targets_ref[...], image), 0.0)
        ),
    )
    send_ref[:, 0:256] = jnp.broadcast_to(along, (send_ref.shape[0], 256))
    send_ref[:, 256:384] = jnp.broadcast_to(sums, (send_ref.shape[0], 128))


def second_body(
    parts_ref, state_ref, image_ref, inverse_ref, sketch_ref, targets_ref, ridge_ref, next_ref, send_ref
):
    sums = jnp.sum(parts_ref[...], axis=0, keepdims=True)
    along = sums[:, 0:256]
    curve, image_square, cross = sums[:, 256:257], sums[:, 257:258], sums[:, 258:259]
    ridge = ridge_ref[0, 0]
    descent = state_ref[3:4, :]
    step = descent / curve
    projected = state_ref[1:2, :] - step * along
    solved = times(eight(projected), inverse_ref[...])
    fitted = times(solved, sketch_ref[...], transposed=True)[0:1]
    resid = targets_ref[...] - step * image_ref[0:1, :]
    square = state_ref[2:3, :] - 2.0 * step * cross + step * step * image_square
    fresh = (square - row_dot(projected, solved[0:1])) / ridge
    direction = (resid - fitted) / ridge + fresh / descent * state_ref[0:1, :]
    next_ref[0:1, :] = direction
    next_ref[1:2, :] = step
    next_ref[2:3, :] = fresh
    send_ref[...] = jnp.broadcast_to(direction, send_ref.shape)


def last_image_body(parts_ref, next_ref, ridge_ref, image_ref, send_ref):
    image = jnp.sum(parts_ref[...], axis=0)[0:1] + ridge_ref[0, 0] * next_ref[0:1, :]
    image_ref[...] = eight(image)
    send_ref[...] = jnp.broadcast_to(row_dot(next_ref[0:1, :], image), send_ref.shape)


def finish_body(
    parts_ref, state_ref, next_ref, image_ref, last_ref, targets_ref, coefficients_ref, residual_ref
):
    curve = jnp.sum(parts_ref[...], axis=0, keepdims=True)[:, 0:1]
    step = next_ref[1:2, :]
    last_step = next_ref[2:3, :] / curve
    coefficients_ref[...] = step * state_ref[0:1, :] + last_step * next_ref[0:1, :]
    residual_ref[...] = targets_ref[...] - step * image_ref[0:1, :] - last_step * last_ref[0:1, :]


def local(points, feature_scale, test_matrix, targets, ridge):
    everyone = lax.axis_size(COL_ROW)
    row_devices = lax.axis_size(ROW)
    own, rank = test_matrix.shape
    ridge = ridge.reshape(1, 1)
    targets = targets.reshape(1, own)
    scale = feature_scale.reshape(1, -1)
    parts, copies = call(
        parts_body,
        [shape(own, 128, dtype=BF16), shape(row_devices, own, 128 + rank, dtype=BF16)],
        points,
        scale,
        test_matrix,
        name="parts",
    )
    chips, cores = lax.axis_size("col_0"), lax.axis_size("col_1")
    chunks = {}
    for shift in range(chips):
        for flip in range(cores):
            pairs = [
                (c, (c // 2 + shift) % chips * 2 + (c % 2 ^ flip)) for c in range(chips * cores)
            ]
            chunks[shift, flip] = lax.ppermute(parts, COL, pairs) if shift or flip else parts
    message = exchanged(copies, ROW).reshape(-1, 128 + rank)
    columns = message.shape[0]
    right, norm, test = call(
        columns_body,
        [shape(columns, 256, dtype=BF16), shape(8, columns), shape(columns, rank, dtype=BF16)],
        message,
        name="columns",
    )
    kerns, partial, sent = [], [], []
    for number, shift in enumerate(ORDER):
        left = jnp.concatenate([chunks[shift, 0], chunks[shift, 1]], axis=0)
        if number > 1:
            left, partial[number - 2] = lax.optimization_barrier((left, partial[number - 2]))
        kern, near, other = kernel_block(left, right, norm, test)
        kerns.append(kern)
        swapped = lax.ppermute(other, "col_1", [(0, 1), (1, 0)])
        partial.append(near + swapped if shift else (near, swapped))
    for shift, part in zip(ORDER[:-1], partial):
        pairs = [(c, (c - shift) % chips) for c in range(chips)]
        sent.append(lax.ppermute(part, "col_0", pairs))
    sums = [*partial[-1], *sent]
    sketch, packed = call(
        core_body,
        [shape(own, rank), shape(everyone, 512)],
        *sums,
        test_matrix,
        targets,
        ridge,
        name="core",
    )
    packed = exchanged(packed, COL_ROW)
    packed = call(summed_body, shape(everyone, 512), packed, name="summed")
    packed = exchanged(packed, COL_ROW)
    inverse, state, send = call(
        first_body,
        [shape(rank, rank), shape(8, own), shape(row_devices, own)],
        packed,
        sketch,
        targets,
        ridge,
        name="first",
    )
    product = kernel_times(kerns, exchanged(send, ROW))
    image, send = call(
        image_body,
        [shape(8, own), shape(everyone, 384)],
        exchanged(product, COL),
        state,
        sketch,
        targets,
        ridge,
        name="image",
    )
    following, send = call(
        second_body,
        [shape(8, own), shape(row_devices, own)],
        exchanged(send, COL_ROW),
        state,
        image,
        inverse,
        sketch,
        targets,
        ridge,
        name="second",
    )
    product = kernel_times(kerns, exchanged(send, ROW))
    last, send = call(
        last_image_body,
        [shape(8, own), shape(everyone, 128)],
        exchanged(product, COL),
        following,
        ridge,
        name="last_image",
    )
    coefficients, residual = call(
        finish_body,
        [shape(1, own), shape(1, own)],
        exchanged(send, COL_ROW),
        state,
        following,
        image,
        last,
        targets,
        name="finish",
    )
    return coefficients.reshape(own), residual.reshape(own), sketch


def solution(mesh):
    split = Mesh(mesh.devices.reshape(4, 4, 4, 2), ROW + COL)
    return jax.shard_map(
        local,
        mesh=split,
        in_specs=(P(COL_ROW, None), P(), P(COL_ROW, None), P(COL_ROW), P()),
        out_specs=(P(COL_ROW), P(COL_ROW), P(COL_ROW, None)),
        check_vma=False,
    )
```

```python
import functools

import jax
import jax.numpy as jnp
from jax import lax
from jax.experimental import pallas as pl
from jax.experimental.pallas import tpu as pltpu
from jax.sharding import Mesh
from jax.sharding import PartitionSpec as P


ROW = ("row_0", "row_1")
COL = ("col_0", "col_1")
COL_ROW = ("col_0", "col_1", "row_0", "row_1")
LOG2E = 1.4426950408889634
MIB = 1024 * 1024
F32 = jnp.float32
BF16 = jnp.bfloat16
HIGH = lax.Precision.HIGHEST
KERN_SPACE = pltpu.VMEM
ORDER = (2, 1, 3, 0)
LATE = ((0, 1), (3, 1))
KLIMIT = 4
KLIMIT2 = 4


def call(body, outs, *args, scratch=(), limit=4):
    return pl.pallas_call(
        body,
        out_shape=outs,
        scratch_shapes=list(scratch),
        compiler_params=pltpu.CompilerParams(vmem_limit_bytes=limit * MIB),
    )(*args)


def shape(*dims, dtype=F32):
    return jax.ShapeDtypeStruct(dims, dtype)


def exchanged(pieces, axes):
    return lax.all_to_all(pieces, axes, 0, 0, tiled=True)


def split3(value):
    first = value.astype(BF16)
    rest = value - first.astype(F32)
    second = rest.astype(BF16)
    third = (rest - second.astype(F32)).astype(BF16)
    return first, second, third


def parts_body(points_ref, scale_ref, test_ref, out_ref, copies_ref):
    y = points_ref[...] * (scale_ref[...] * LOG2E**0.5)
    first = y.astype(BF16).astype(F32)
    second = (y - first).astype(BF16).astype(F32)
    parts = jnp.concatenate([first, second], axis=1).astype(BF16)
    out_ref[...] = parts
    for i in range(copies_ref.shape[0]):
        copies_ref[i, :, 0:128] = parts
        copies_ref[i, :, 128:384] = test_ref[...]


def norms_body(message_ref, norm_ref):
    lane = lax.broadcasted_iota(jnp.int32, (128, 128), 1)
    sub = lax.broadcasted_iota(jnp.int32, (128, 128), 0)
    twice = jnp.where((lane - sub) % 64 == 0, 1.0, 0.0).astype(BF16)
    points = jnp.dot(message_ref[:, 0:128], twice, preferred_element_type=F32)
    squares = -0.25 * (points * points)
    lane8, sub8 = lane[0:8], sub[0:8]
    for base in range(0, message_ref.shape[0], 128):
        packed = jnp.zeros((8, 128), F32)
        for at in range(0, 128, 8):
            total = jnp.sum(squares[base + at : base + at + 8], axis=1, keepdims=True)
            packed = packed + jnp.where(lane8 == sub8 + at, total, 0.0)
        norm_ref[:, base : base + 128] = eight(jnp.sum(packed, axis=0, keepdims=True))


def block_body(first_ref, second_ref, message_ref, norm_ref, kern_ref, own_ref, other_ref, *, chunk):
    parts = jnp.concatenate([first_ref[...], second_ref[...]], axis=0)
    turned = pltpu.roll(parts.astype(F32), 64, 1)
    points = parts.astype(F32) + turned
    left_norm = -0.25 * jnp.sum(points * points, axis=1, keepdims=True)
    left = jnp.concatenate([parts, turned.astype(BF16)], axis=1)
    total = None
    for start in range(0, message_ref.shape[0], chunk):
        span = slice(start, start + chunk)
        right = message_ref[span, 0:128]
        exponent = lax.dot_general(
            left,
            jnp.concatenate([right, right], axis=1),
            (((1,), (1,)), ((), ())),
            preferred_element_type=F32,
        )
        weights = jnp.exp2(exponent + left_norm + norm_ref[0:1, span])
        kern_ref[:, span] = weights
        part = jnp.dot(
            weights.astype(BF16), message_ref[span, 128:], preferred_element_type=F32
        )
        total = part if total is None else total + part
    half = total.shape[0] // 2
    own_ref[...] = total[:half]
    other_ref[...] = total[half:]


def kernel_block(first, second, message, norm):
    rows, columns, rank = first.shape[0], message.shape[0], message.shape[1] - 128
    return call(
        functools.partial(block_body, chunk=512),
        [KERN_SPACE((2 * rows, columns), F32), shape(rows, rank), shape(rows, rank)],
        first,
        second,
        message,
        norm,
        limit=KLIMIT,
    )


def core_body(
    near_ref, swapped_ref, one_ref, two_ref, three_ref, test_ref, targets_ref, ridge_ref, sketch_ref, copy_ref, out_ref
):
    sketch = near_ref[...] + swapped_ref[...] + one_ref[...] + two_ref[...] + three_ref[...]
    sketch_ref[...] = sketch
    copy_ref[...] = sketch
    shifted = ridge_ref[0, 0] * test_ref[...].astype(F32) + sketch
    core = lax.dot_general(
        shifted, sketch, (((0,), (0,)), ((), ())), precision=HIGH, preferred_element_type=F32
    )
    targets = jnp.broadcast_to(targets_ref[...], (8, 256))
    projected = jnp.dot(targets, sketch, precision=HIGH, preferred_element_type=F32)
    square = jnp.sum(targets[0:1] * targets[0:1], axis=1, keepdims=True)
    row = lax.broadcasted_iota(jnp.int32, (8, 128), 0)
    extra = jnp.where(row == 2, square, 0.0)
    extra = jnp.where(row == 1, projected[:, 128:256], extra)
    extra = jnp.where(row == 0, projected[:, 0:128], extra)
    out_ref[:, 0:256] = core[0:128]
    out_ref[:, 256:384] = core[128:256, 128:256]
    out_ref[:, 384:512] = jnp.zeros((128, 128), F32)
    out_ref[0:8, 384:512] = extra


def summed_body(parts_ref, out_ref):
    out_ref[...] = jnp.broadcast_to(jnp.sum(parts_ref[...], axis=0, keepdims=True), out_ref.shape)


def inverted(work_ref):
    size = work_ref.shape[0]
    panels = size // 8
    sub = lax.broadcasted_iota(jnp.int32, (8, 1), 0)
    lanes = lax.broadcasted_iota(jnp.int32, (1, size), 1)

    def column(block, step, j):
        index = jnp.full((8, 128), 0, jnp.int32) + ((step % 16) * 8 + j)
        window = jnp.where(step < 16, block[:, 0:128], block[:, 128:256])
        return jnp.take_along_axis(window, index, axis=1)

    def wide(value):
        return jnp.concatenate([value, value], axis=1)

    def eliminated(panel, step):
        diag = [column(panel, step, j) for j in range(8)]
        for j in range(8):
            inverse = 1.0 / diag[j][j : j + 1, :]
            for k in range(j + 1, 8):
                pivot = diag[k][j : j + 1, :] * inverse
                diag[k] = jnp.where(sub == j, pivot, diag[k] - diag[j] * pivot)
            panel = jnp.where(lanes == step * 8 + j, jnp.where(sub == j, 1.0, 0.0), panel)
            row = panel[j : j + 1, :] * wide(inverse)
            panel = jnp.where(sub == j, row, panel - wide(diag[j]) * row)
        return panel

    def split(value):
        return [part.astype(F32) for part in split3(value)]

    def stacked(parts):
        return jnp.concatenate(parts, axis=0).astype(BF16)

    def panel_step(step, carry):
        panel, factors = carry
        following = jnp.minimum(step + 1, panels - 1)
        here = pl.ds(pl.multiple_of(step * 8, 8), 8)
        ahead = work_ref[pl.ds(pl.multiple_of(following * 8, 8), 8), :]
        inside = (lanes >= step * 8) & (lanes < step * 8 + 8)
        following_rows = jnp.where(inside, 0.0, ahead)
        for j in range(8):
            following_rows = following_rows - wide(column(ahead, step, j)) * panel[j : j + 1, :]
        f1, f2, f3 = split(factors)
        p1, p2, p3 = split(panel)
        update = lax.dot_general(
            stacked([f1, f1, f2, f2, f1, f3]),
            stacked([p1, p2, p1, p2, p3, p1]),
            (((0,), (0,)), ((), ())),
            preferred_element_type=F32,
        )
        work_ref[...] = jnp.where(inside, 0.0, work_ref[...]) - update
        work_ref[here, :] = panel
        following_factors = jnp.where(lanes < following * 8, -following_rows, following_rows)
        return eliminated(following_rows, following), following_factors

    start = work_ref[0:8, :]
    lax.fori_loop(0, panels, panel_step, (eliminated(start, 0), start))


def eight(row):
    return jnp.broadcast_to(row, (8, row.shape[1]))


def row_dot(a, b):
    return jnp.sum(a * b, axis=1, keepdims=True)


def times(vector, matrix, transposed=False):
    dims = (((1,), (1 if transposed else 0,)), ((), ()))
    return lax.dot_general(vector, matrix, dims, precision=HIGH, preferred_element_type=F32)


def first_body(packed_ref, sketch_ref, targets_ref, ridge_ref, inverse_ref, state_ref, send_ref):
    inverse_ref[0:128, :] = packed_ref[:, 0:256]
    inverse_ref[128:256, 0:128] = packed_ref[:, 128:256].T
    inverse_ref[128:256, 128:256] = packed_ref[:, 256:384]
    inverted(inverse_ref)
    projected = jnp.concatenate([packed_ref[0:1, 384:512], packed_ref[1:2, 384:512]], axis=1)
    square = packed_ref[2:3, 384:385]
    solved = times(eight(projected), inverse_ref[...])
    fitted = times(solved, sketch_ref[...], transposed=True)
    ridge = ridge_ref[0, 0]
    direction = (targets_ref[...] - fitted[0:1]) / ridge
    descent = (square - row_dot(projected, solved[0:1])) / ridge
    state_ref[0:1, :] = direction
    state_ref[1:2, :] = projected
    state_ref[2:3, :] = jnp.broadcast_to(square, (1, 256))
    state_ref[3:4, :] = jnp.broadcast_to(descent, (1, 256))
    send_ref[...] = jnp.broadcast_to(direction, send_ref.shape)


def products(kern_refs, vector):
    tiles = kern_refs[0].shape[1] // 128
    sub = lax.broadcasted_iota(jnp.int32, (8, 128), 0)
    lane = lax.broadcasted_iota(jnp.int32, (8, 128), 1)
    chip, core = lax.axis_index("col_0"), lax.axis_index("col_1")
    chips = len(kern_refs)
    for shift, kern_ref in zip(ORDER, kern_refs):
        for flip in range(2):
            place = (chip + (chips - shift)) % chips * 2 + (core + flip) % 2
            for half in range(2):
                packed = jnp.zeros((8, 128), F32)
                for start in range(0, 128, 64):
                    base = flip * 256 + half * 128 + start
                    acc = [None] * 8
                    for k in range(tiles):
                        span = slice(k % 2 * 128, k % 2 * 128 + 128)
                        piece = eight(vector[k // 2 : k // 2 + 1, span])
                        for g in range(8):
                            block = kern_ref[
                                base + g * 8 : base + g * 8 + 8, k * 128 : k * 128 + 128
                            ]
                            acc[g] = block * piece if k == 0 else acc[g] + block * piece
                    for g in range(8):
                        total = jnp.sum(acc[g], axis=1, keepdims=True)
                        packed = packed + jnp.where(lane == sub + (start + g * 8), total, 0.0)
                yield place, half, jnp.sum(packed, axis=0, keepdims=True)


def product_body(*refs):
    *kern_refs, vector_ref, out_ref = refs
    for place, half, piece in products(kern_refs, vector_ref):
        out_ref[place, :, half * 128 : half * 128 + 128] = eight(piece)


def last_product_body(*refs):
    *kern_refs, vector_ref, out_ref = refs
    rows = out_ref.shape[0] // 8
    own_place = lax.axis_index("col_0") * 2 + lax.axis_index("col_1")
    own_row = lax.axis_index("row_0") * 4 + lax.axis_index("row_1")
    mine = lax.broadcasted_iota(jnp.int32, (rows, 128), 0) == own_row
    curve = jnp.zeros((rows, 128), F32)

    def group(place):
        return pl.ds(pl.multiple_of(place * rows, rows), rows)

    for place, half, piece in products(kern_refs, vector_ref[group(own_place), :]):
        span = slice(half * 128, half * 128 + 128)
        curve = curve + piece * jnp.where(mine, vector_ref[group(place), span], 0.0)
        out_ref[group(place), span] = jnp.broadcast_to(piece, (rows, 128))
    curve = jnp.sum(curve, axis=0, keepdims=True)
    out_ref[:, 256:384] = jnp.broadcast_to(curve, (out_ref.shape[0], 128))


def kernel_times(kerns, vector):
    return call(product_body, shape(8, 8, 256), *kerns, vector, limit=KLIMIT2)


def image_body(parts_ref, state_ref, sketch_ref, targets_ref, ridge_ref, image_ref, send_ref):
    image = jnp.sum(parts_ref[...], axis=0)[0:1] + ridge_ref[0, 0] * state_ref[0:1, :]
    image_ref[...] = eight(image)
    along = times(eight(image), sketch_ref[...])[0:1]
    lane = lax.broadcasted_iota(jnp.int32, (1, 128), 1)
    sums = jnp.where(
        lane == 0,
        row_dot(state_ref[0:1, :], image),
        jnp.where(
            lane == 1, row_dot(image, image), jnp.where(lane == 2, row_dot(targets_ref[...], image), 0.0)
        ),
    )
    send_ref[:, 0:256] = jnp.broadcast_to(along, (send_ref.shape[0], 256))
    send_ref[:, 256:384] = jnp.broadcast_to(sums, (send_ref.shape[0], 128))


def second_body(
    parts_ref, state_ref, image_ref, inverse_ref, sketch_ref, targets_ref, ridge_ref, next_ref, send_ref
):
    sums = jnp.sum(parts_ref[...], axis=0, keepdims=True)
    along = sums[:, 0:256]
    curve, image_square, cross = sums[:, 256:257], sums[:, 257:258], sums[:, 258:259]
    ridge = ridge_ref[0, 0]
    descent = state_ref[3:4, :]
    step = descent / curve
    projected = state_ref[1:2, :] - step * along
    solved = times(eight(projected), inverse_ref[...])
    fitted = times(solved, sketch_ref[...], transposed=True)[0:1]
    resid = targets_ref[...] - step * image_ref[0:1, :]
    square = state_ref[2:3, :] - 2.0 * step * cross + step * step * image_square
    fresh = (square - row_dot(projected, solved[0:1])) / ridge
    direction = (resid - fitted) / ridge + fresh / descent * state_ref[0:1, :]
    next_ref[0:1, :] = direction
    next_ref[1:2, :] = step
    next_ref[2:3, :] = fresh
    send_ref[...] = jnp.broadcast_to(direction, send_ref.shape)


def finish_body(
    parts_ref,
    every_ref,
    state_ref,
    next_ref,
    image_ref,
    targets_ref,
    ridge_ref,
    coefficients_ref,
    residual_ref,
):
    ridge = ridge_ref[0, 0]
    own_row = lax.axis_index("row_0") * 4 + lax.axis_index("row_1")
    rows = parts_ref.shape[0] // 8
    direction = next_ref[0:1, :]
    mine = lax.broadcasted_iota(jnp.int32, (8 * rows, 256), 0) % rows == own_row
    last = jnp.sum(jnp.where(mine, parts_ref[:, 0:256], 0.0), axis=0, keepdims=True)
    last = last + ridge * direction
    every = every_ref[...]
    square = jnp.sum(jnp.sum(every * every, axis=0, keepdims=True), axis=1, keepdims=True)
    curve = jnp.sum(
        jnp.sum(parts_ref[:, 256:384], axis=0, keepdims=True), axis=1, keepdims=True
    )
    step = next_ref[1:2, :]
    last_step = next_ref[2:3, :] / (curve + ridge * square)
    coefficients_ref[...] = step * state_ref[0:1, :] + last_step * direction
    residual_ref[...] = targets_ref[...] - step * image_ref[0:1, :] - last_step * last


def local(points, feature_scale, test_matrix, targets, ridge):
    everyone = lax.axis_size(COL_ROW)
    row_devices = lax.axis_size(ROW)
    own, rank = test_matrix.shape
    ridge = ridge.reshape(1, 1)
    targets = targets.reshape(1, own)
    scale = feature_scale.reshape(1, -1)
    parts, copies = call(
        parts_body,
        [shape(own, 128, dtype=BF16), shape(row_devices, own, 128 + rank, dtype=BF16)],
        points,
        scale,
        test_matrix,
    )
    chips, cores = lax.axis_size("col_0"), lax.axis_size("col_1")
    chunks = {}
    for shift in range(chips):
        for flip in range(cores):
            pairs = [
                (c, (c // 2 + shift) % chips * 2 + (c % 2 ^ flip)) for c in range(chips * cores)
            ]
            chunks[shift, flip] = lax.ppermute(parts, COL, pairs) if shift or flip else parts
    message = exchanged(copies, ROW).reshape(-1, 128 + rank)
    early = {key: value for key, value in chunks.items() if key not in LATE}
    message, early = lax.optimization_barrier((message, early))
    chunks.update(early)
    norm = call(norms_body, shape(8, message.shape[0]), message)
    kerns, partial, sent = [], [], []
    for number, shift in enumerate(ORDER):
        first = chunks[shift, 0]
        if number > 1:
            first, partial[number - 2] = lax.optimization_barrier((first, partial[number - 2]))
        kern, near, other = kernel_block(first, chunks[shift, 1], message, norm)
        kerns.append(kern)
        swapped = lax.ppermute(other, "col_1", [(0, 1), (1, 0)])
        partial.append(near + swapped if shift else (near, swapped))
    for number, shift in enumerate(ORDER[:-1]):
        pairs = [(c, (c - shift) % chips) for c in range(chips)]
        sent.append(lax.ppermute(partial[number], "col_0", pairs))
    sums = [*partial[-1], *sent]
    sketch_out, sketch, packed = call(
        core_body,
        [shape(own, rank), shape(own, rank), shape(everyone, 512)],
        *sums,
        test_matrix,
        targets,
        ridge,
    )
    packed = exchanged(packed, COL_ROW)
    packed = call(summed_body, shape(everyone, 512), packed)
    packed = exchanged(packed, COL_ROW)
    inverse, state, send = call(
        first_body,
        [shape(rank, rank), shape(8, own), shape(row_devices, own)],
        packed,
        sketch,
        targets,
        ridge,
    )
    product = kernel_times(kerns, exchanged(send, ROW))
    image, send = call(
        image_body,
        [shape(8, own), shape(everyone, 384)],
        exchanged(product, COL),
        state,
        sketch,
        targets,
        ridge,
    )
    following, send = call(
        second_body,
        [shape(8, own), shape(everyone, own)],
        exchanged(send, COL_ROW),
        state,
        image,
        inverse,
        sketch,
        targets,
        ridge,
    )
    every = exchanged(send, COL_ROW)
    product = call(last_product_body, shape(everyone, 384), *kerns, every, limit=KLIMIT2)
    coefficients, residual = call(
        finish_body,
        [shape(1, own), shape(1, own)],
        exchanged(product, COL_ROW),
        every,
        state,
        following,
        image,
        targets,
        ridge,
    )
    return coefficients.reshape(own), residual.reshape(own), sketch_out


def solution(mesh):
    split = Mesh(mesh.devices.reshape(4, 4, 4, 2), ROW + COL)

    return jax.shard_map(
        local,
        mesh=split,
        in_specs=(P(COL_ROW, None), P(), P(COL_ROW, None), P(COL_ROW), P()),
        out_specs=(P(COL_ROW), P(COL_ROW), P(COL_ROW, None)),
        check_vma=False,
    )
```

```python
import functools

import jax
import jax.numpy as jnp
from jax import lax
from jax.experimental import pallas as pl
from jax.experimental.pallas import tpu as pltpu
from jax.sharding import Mesh
from jax.sharding import PartitionSpec as P


ROW = ("row_0", "row_1")
COL = ("col_0", "col_1")
COL_ROW = ("col_0", "col_1", "row_0", "row_1")
LOG2E = 1.4426950408889634
MIB = 1024 * 1024
F32 = jnp.float32
BF16 = jnp.bfloat16
HIGH = lax.Precision.HIGHEST
KERN_SPACE = pltpu.VMEM
ORDER = (2, 1, 3, 0)
LATE = ((0, 1), (3, 1))
KLIMIT = 4
KLIMIT2 = 4


def call(body, outs, *args, scratch=(), limit=4):
    return pl.pallas_call(
        body,
        out_shape=outs,
        scratch_shapes=list(scratch),
        compiler_params=pltpu.CompilerParams(vmem_limit_bytes=limit * MIB),
    )(*args)


def shape(*dims, dtype=F32):
    return jax.ShapeDtypeStruct(dims, dtype)


def exchanged(pieces, axes):
    return lax.all_to_all(pieces, axes, 0, 0, tiled=True)


def split3(value):
    first = value.astype(BF16)
    rest = value - first.astype(F32)
    second = rest.astype(BF16)
    third = (rest - second.astype(F32)).astype(BF16)
    return first, second, third


def parts_body(
    points_ref, scale_ref, test_ref, out_ref, copies_ref, points_scr, scale_scr, message_scr, in_sem, out_sem
):
    inputs = (
        (points_ref, points_scr),
        (scale_ref, scale_scr),
        (test_ref, message_scr.at[:, 128:384]),
    )
    loads = [pltpu.make_async_copy(*pair, in_sem.at[i]) for i, pair in enumerate(inputs)]
    for load in loads:
        load.start()
    loads[0].wait()
    loads[1].wait()
    y = points_scr[...].T * (scale_scr[...] * LOG2E**0.5)
    first = y.astype(BF16).astype(F32)
    second = (y - first).astype(BF16).astype(F32)
    parts = jnp.concatenate([first, second], axis=1).astype(BF16)
    out_ref[...] = parts
    message_scr[:, 0:128] = parts
    loads[2].wait()
    stores = [
        pltpu.make_async_copy(message_scr, copies_ref.at[i], out_sem.at[i])
        for i in range(copies_ref.shape[0])
    ]
    for store in stores:
        store.start()
    for store in stores:
        store.wait()


def parts_and_copies(points, scale, test, copies):
    own, features = points.shape
    lanes = 128 + test.shape[1]
    anywhere = pl.BlockSpec(memory_space=pltpu.HBM)
    return pl.pallas_call(
        parts_body,
        in_specs=[anywhere] * 3,
        out_specs=[pl.BlockSpec(memory_space=pltpu.VMEM), anywhere],
        out_shape=[shape(own, 128, dtype=BF16), pltpu.HBM((copies, own, lanes), BF16)],
        scratch_shapes=[
            pltpu.VMEM((features, own), F32),
            pltpu.VMEM((1, features), F32),
            pltpu.VMEM((own, lanes), BF16),
            pltpu.SemaphoreType.DMA((3,)),
            pltpu.SemaphoreType.DMA((copies,)),
        ],
        compiler_params=pltpu.CompilerParams(vmem_limit_bytes=4 * MIB),
        name="parts",
    )(*(pltpu.with_memory_space_constraint(a, pltpu.HBM) for a in (points.T, scale, test)))


def norms_body(message_ref, norm_ref):
    lane = lax.broadcasted_iota(jnp.int32, (128, 128), 1)
    sub = lax.broadcasted_iota(jnp.int32, (128, 128), 0)
    twice = jnp.where((lane - sub) % 64 == 0, 1.0, 0.0).astype(BF16)
    points = jnp.dot(message_ref[:, 0:128], twice, preferred_element_type=F32)
    squares = -0.25 * (points * points)
    lane8, sub8 = lane[0:8], sub[0:8]
    for base in range(0, message_ref.shape[0], 128):
        packed = jnp.zeros((8, 128), F32)
        for at in range(0, 128, 8):
            total = jnp.sum(squares[base + at : base + at + 8], axis=1, keepdims=True)
            packed = packed + jnp.where(lane8 == sub8 + at, total, 0.0)
        norm_ref[:, base : base + 128] = eight(jnp.sum(packed, axis=0, keepdims=True))


def block_body(first_ref, second_ref, message_ref, norm_ref, kern_ref, own_ref, other_ref, *, chunk):
    parts = jnp.concatenate([first_ref[...], second_ref[...]], axis=0)
    turned = pltpu.roll(parts.astype(F32), 64, 1)
    points = parts.astype(F32) + turned
    left_norm = -0.25 * jnp.sum(points * points, axis=1, keepdims=True)
    left = jnp.concatenate([parts, turned.astype(BF16)], axis=1)
    total = None
    for start in range(0, message_ref.shape[0], chunk):
        span = slice(start, start + chunk)
        right = message_ref[span, 0:128]
        exponent = lax.dot_general(
            left,
            jnp.concatenate([right, right], axis=1),
            (((1,), (1,)), ((), ())),
            preferred_element_type=F32,
        )
        weights = jnp.exp2(exponent + left_norm + norm_ref[0:1, span])
        kern_ref[:, span] = weights
        part = jnp.dot(
            weights.astype(BF16), message_ref[span, 128:], preferred_element_type=F32
        )
        total = part if total is None else total + part
    half = total.shape[0] // 2
    own_ref[...] = total[:half]
    other_ref[...] = total[half:]


def kernel_block(first, second, message, norm):
    rows, columns, rank = first.shape[0], message.shape[0], message.shape[1] - 128
    return call(
        functools.partial(block_body, chunk=512),
        [KERN_SPACE((2 * rows, columns), F32), shape(rows, rank), shape(rows, rank)],
        first,
        second,
        message,
        norm,
        limit=KLIMIT,
    )


def core_body(
    near_ref, swapped_ref, one_ref, two_ref, three_ref, test_ref, targets_ref, ridge_ref, sketch_ref, copy_ref, out_ref
):
    sketch = near_ref[...] + swapped_ref[...] + one_ref[...] + two_ref[...] + three_ref[...]
    sketch_ref[...] = sketch
    copy_ref[...] = sketch
    shifted = ridge_ref[0, 0] * test_ref[...].astype(F32) + sketch
    core = lax.dot_general(
        shifted, sketch, (((0,), (0,)), ((), ())), precision=HIGH, preferred_element_type=F32
    )
    targets = jnp.broadcast_to(targets_ref[...], (8, 256))
    projected = jnp.dot(targets, sketch, precision=HIGH, preferred_element_type=F32)
    square = jnp.sum(targets[0:1] * targets[0:1], axis=1, keepdims=True)
    row = lax.broadcasted_iota(jnp.int32, (8, 128), 0)
    extra = jnp.where(row == 2, square, 0.0)
    extra = jnp.where(row == 1, projected[:, 128:256], extra)
    extra = jnp.where(row == 0, projected[:, 0:128], extra)
    out_ref[:, 0:256] = core[0:128]
    out_ref[:, 256:384] = core[128:256, 128:256]
    out_ref[:, 384:512] = jnp.zeros((128, 128), F32)
    out_ref[0:8, 384:512] = extra


def summed_body(parts_ref, out_ref):
    out_ref[...] = jnp.broadcast_to(jnp.sum(parts_ref[...], axis=0, keepdims=True), out_ref.shape)


def inverted(work_ref):
    size = work_ref.shape[0]
    panels = size // 8
    sub = lax.broadcasted_iota(jnp.int32, (8, 1), 0)
    lanes = lax.broadcasted_iota(jnp.int32, (1, size), 1)

    def column(block, step, j):
        index = jnp.full((8, 128), 0, jnp.int32) + ((step % 16) * 8 + j)
        window = jnp.where(step < 16, block[:, 0:128], block[:, 128:256])
        return jnp.take_along_axis(window, index, axis=1)

    def wide(value):
        return jnp.concatenate([value, value], axis=1)

    def eliminated(panel, step):
        diag = [column(panel, step, j) for j in range(8)]
        for j in range(0, 8, 2):
            a, b = diag[j][j : j + 1, :], diag[j + 1][j : j + 1, :]
            c, d = diag[j][j + 1 : j + 2, :], diag[j + 1][j + 1 : j + 2, :]
            inverse = 1.0 / (a * d - b * c)
            upper, lower = sub == j, sub == j + 1

            def swept(block, first, second, spread=lambda value: value):
                top, bottom = block[j : j + 1, :], block[j + 1 : j + 2, :]
                new_top = (spread(d) * top - spread(b) * bottom) * spread(inverse)
                new_bottom = (spread(a) * bottom - spread(c) * top) * spread(inverse)
                rest = block - first * new_top - second * new_bottom
                return jnp.where(upper, new_top, jnp.where(lower, new_bottom, rest))

            for k in range(j + 2, 8):
                diag[k] = swept(diag[k], diag[j], diag[j + 1])
            panel = jnp.where(lanes == step * 8 + j, jnp.where(upper, 1.0, 0.0), panel)
            panel = jnp.where(lanes == step * 8 + j + 1, jnp.where(lower, 1.0, 0.0), panel)
            panel = swept(panel, wide(diag[j]), wide(diag[j + 1]), wide)
        return panel

    def split(value):
        return [part.astype(F32) for part in split3(value)]

    def stacked(parts):
        return jnp.concatenate(parts, axis=0).astype(BF16)

    def panel_step(step, carry):
        panel, factors = carry
        following = jnp.minimum(step + 1, panels - 1)
        here = pl.ds(pl.multiple_of(step * 8, 8), 8)
        ahead = work_ref[pl.ds(pl.multiple_of(following * 8, 8), 8), :]
        inside = (lanes >= step * 8) & (lanes < step * 8 + 8)
        following_rows = jnp.where(inside, 0.0, ahead)
        for j in range(8):
            following_rows = following_rows - wide(column(ahead, step, j)) * panel[j : j + 1, :]
        f1, f2, f3 = split(factors)
        p1, p2, p3 = split(panel)
        update = lax.dot_general(
            stacked([f1, f1, f2, f2, f1, f3]),
            stacked([p1, p2, p1, p2, p3, p1]),
            (((0,), (0,)), ((), ())),
            preferred_element_type=F32,
        )
        work_ref[...] = jnp.where(inside, 0.0, work_ref[...]) - update
        work_ref[here, :] = panel
        following_factors = jnp.where(lanes < following * 8, -following_rows, following_rows)
        return eliminated(following_rows, following), following_factors

    start = work_ref[0:8, :]
    lax.fori_loop(0, panels, panel_step, (eliminated(start, 0), start))


def eight(row):
    return jnp.broadcast_to(row, (8, row.shape[1]))


def row_dot(a, b):
    return jnp.sum(a * b, axis=1, keepdims=True)


def times(vector, matrix, transposed=False):
    dims = (((1,), (1 if transposed else 0,)), ((), ()))
    return lax.dot_general(vector, matrix, dims, precision=HIGH, preferred_element_type=F32)


def first_body(packed_ref, sketch_ref, targets_ref, ridge_ref, inverse_ref, state_ref, send_ref):
    inverse_ref[0:128, :] = packed_ref[:, 0:256]
    inverse_ref[128:256, 0:128] = packed_ref[:, 128:256].T
    inverse_ref[128:256, 128:256] = packed_ref[:, 256:384]
    inverted(inverse_ref)
    projected = jnp.concatenate([packed_ref[0:1, 384:512], packed_ref[1:2, 384:512]], axis=1)
    square = packed_ref[2:3, 384:385]
    solved = times(eight(projected), inverse_ref[...])
    fitted = times(solved, sketch_ref[...], transposed=True)
    ridge = ridge_ref[0, 0]
    direction = (targets_ref[...] - fitted[0:1]) / ridge
    descent = (square - row_dot(projected, solved[0:1])) / ridge
    state_ref[0:1, :] = direction
    state_ref[1:2, :] = projected
    state_ref[2:3, :] = jnp.broadcast_to(square, (1, 256))
    state_ref[3:4, :] = jnp.broadcast_to(descent, (1, 256))
    send_ref[...] = jnp.broadcast_to(direction, send_ref.shape)


def products(kern_refs, vector):
    tiles = kern_refs[0].shape[1] // 128
    sub = lax.broadcasted_iota(jnp.int32, (8, 128), 0)
    lane = lax.broadcasted_iota(jnp.int32, (8, 128), 1)
    chip, core = lax.axis_index("col_0"), lax.axis_index("col_1")
    chips = len(kern_refs)
    for shift, kern_ref in zip(ORDER, kern_refs):
        for flip in range(2):
            place = (chip + (chips - shift)) % chips * 2 + (core + flip) % 2
            for half in range(2):
                packed = jnp.zeros((8, 128), F32)
                for start in range(0, 128, 64):
                    base = flip * 256 + half * 128 + start
                    acc = [None] * 8
                    for k in range(tiles):
                        span = slice(k % 2 * 128, k % 2 * 128 + 128)
                        piece = eight(vector[k // 2 : k // 2 + 1, span])
                        for g in range(8):
                            block = kern_ref[
                                base + g * 8 : base + g * 8 + 8, k * 128 : k * 128 + 128
                            ]
                            acc[g] = block * piece if k == 0 else acc[g] + block * piece
                    for g in range(8):
                        total = jnp.sum(acc[g], axis=1, keepdims=True)
                        packed = packed + jnp.where(lane == sub + (start + g * 8), total, 0.0)
                yield place, half, jnp.sum(packed, axis=0, keepdims=True)


def product_body(*refs):
    *kern_refs, vector_ref, out_ref = refs
    for place, half, piece in products(kern_refs, vector_ref):
        out_ref[place, :, half * 128 : half * 128 + 128] = eight(piece)


def last_product_body(*refs):
    *kern_refs, vector_ref, out_ref = refs
    rows = out_ref.shape[0] // 8
    own_place = lax.axis_index("col_0") * 2 + lax.axis_index("col_1")
    own_row = lax.axis_index("row_0") * 4 + lax.axis_index("row_1")
    mine = lax.broadcasted_iota(jnp.int32, (rows, 128), 0) == own_row
    curve = jnp.zeros((rows, 128), F32)

    def group(place):
        return pl.ds(pl.multiple_of(place * rows, rows), rows)

    for place, half, piece in products(kern_refs, vector_ref[group(own_place), :]):
        span = slice(half * 128, half * 128 + 128)
        curve = curve + piece * jnp.where(mine, vector_ref[group(place), span], 0.0)
        out_ref[group(place), span] = jnp.broadcast_to(piece, (rows, 128))
    curve = jnp.sum(curve, axis=0, keepdims=True)
    out_ref[:, 256:384] = jnp.broadcast_to(curve, (out_ref.shape[0], 128))


def kernel_times(kerns, vector):
    return call(product_body, shape(8, 8, 256), *kerns, vector, limit=KLIMIT2)


def image_body(parts_ref, state_ref, sketch_ref, targets_ref, ridge_ref, image_ref, send_ref):
    image = jnp.sum(parts_ref[...], axis=0)[0:1] + ridge_ref[0, 0] * state_ref[0:1, :]
    image_ref[...] = eight(image)
    along = times(eight(image), sketch_ref[...])[0:1]
    lane = lax.broadcasted_iota(jnp.int32, (1, 128), 1)
    sums = jnp.where(
        lane == 0,
        row_dot(state_ref[0:1, :], image),
        jnp.where(
            lane == 1, row_dot(image, image), jnp.where(lane == 2, row_dot(targets_ref[...], image), 0.0)
        ),
    )
    send_ref[:, 0:256] = jnp.broadcast_to(along, (send_ref.shape[0], 256))
    send_ref[:, 256:384] = jnp.broadcast_to(sums, (send_ref.shape[0], 128))


def second_body(
    parts_ref, state_ref, image_ref, inverse_ref, sketch_ref, targets_ref, ridge_ref, next_ref, send_ref
):
    sums = jnp.sum(parts_ref[...], axis=0, keepdims=True)
    along = sums[:, 0:256]
    curve, image_square, cross = sums[:, 256:257], sums[:, 257:258], sums[:, 258:259]
    ridge = ridge_ref[0, 0]
    descent = state_ref[3:4, :]
    step = descent / curve
    projected = state_ref[1:2, :] - step * along
    solved = times(eight(projected), inverse_ref[...])
    fitted = times(solved, sketch_ref[...], transposed=True)[0:1]
    resid = targets_ref[...] - step * image_ref[0:1, :]
    square = state_ref[2:3, :] - 2.0 * step * cross + step * step * image_square
    fresh = (square - row_dot(projected, solved[0:1])) / ridge
    direction = (resid - fitted) / ridge + fresh / descent * state_ref[0:1, :]
    next_ref[0:1, :] = direction
    next_ref[1:2, :] = step
    next_ref[2:3, :] = fresh
    send_ref[...] = jnp.broadcast_to(direction, send_ref.shape)


def finish_body(
    parts_ref,
    every_ref,
    state_ref,
    next_ref,
    image_ref,
    targets_ref,
    ridge_ref,
    coefficients_ref,
    residual_ref,
):
    ridge = ridge_ref[0, 0]
    own_row = lax.axis_index("row_0") * 4 + lax.axis_index("row_1")
    rows = parts_ref.shape[0] // 8
    direction = next_ref[0:1, :]
    mine = lax.broadcasted_iota(jnp.int32, (8 * rows, 256), 0) % rows == own_row
    last = jnp.sum(jnp.where(mine, parts_ref[:, 0:256], 0.0), axis=0, keepdims=True)
    last = last + ridge * direction
    every = every_ref[...]
    square = jnp.sum(jnp.sum(every * every, axis=0, keepdims=True), axis=1, keepdims=True)
    curve = jnp.sum(
        jnp.sum(parts_ref[:, 256:384], axis=0, keepdims=True), axis=1, keepdims=True
    )
    step = next_ref[1:2, :]
    last_step = next_ref[2:3, :] / (curve + ridge * square)
    coefficients_ref[...] = step * state_ref[0:1, :] + last_step * direction
    residual_ref[...] = targets_ref[...] - step * image_ref[0:1, :] - last_step * last


def local(points, feature_scale, test_matrix, targets, ridge):
    everyone = lax.axis_size(COL_ROW)
    row_devices = lax.axis_size(ROW)
    own, rank = test_matrix.shape
    ridge = ridge.reshape(1, 1)
    targets = targets.reshape(1, own)
    scale = feature_scale.reshape(1, -1)
    parts, copies = parts_and_copies(points, scale, test_matrix, row_devices)
    chips, cores = lax.axis_size("col_0"), lax.axis_size("col_1")
    chunks = {}
    for shift in range(chips):
        for flip in range(cores):
            pairs = [
                (c, (c // 2 + shift) % chips * 2 + (c % 2 ^ flip)) for c in range(chips * cores)
            ]
            chunks[shift, flip] = lax.ppermute(parts, COL, pairs) if shift or flip else parts
    message = exchanged(copies, ROW).reshape(-1, 128 + rank)
    early = {key: value for key, value in chunks.items() if key not in LATE}
    message, early = lax.optimization_barrier((message, early))
    chunks.update(early)
    norm = call(norms_body, shape(8, message.shape[0]), message)
    kerns, partial, sent = [], [], []
    for number, shift in enumerate(ORDER):
        first = chunks[shift, 0]
        if number > 1:
            first, partial[number - 2] = lax.optimization_barrier((first, partial[number - 2]))
        kern, near, other = kernel_block(first, chunks[shift, 1], message, norm)
        kerns.append(kern)
        swapped = lax.ppermute(other, "col_1", [(0, 1), (1, 0)])
        partial.append(near + swapped if shift else (near, swapped))
    for number, shift in enumerate(ORDER[:-1]):
        pairs = [(c, (c - shift) % chips) for c in range(chips)]
        sent.append(lax.ppermute(partial[number], "col_0", pairs))
    sums = [*partial[-1], *sent]
    sketch_out, sketch, packed = call(
        core_body,
        [shape(own, rank), shape(own, rank), shape(everyone, 512)],
        *sums,
        test_matrix,
        targets,
        ridge,
    )
    packed = exchanged(packed, COL_ROW)
    packed = call(summed_body, shape(everyone, 512), packed)
    packed = exchanged(packed, COL_ROW)
    inverse, state, send = call(
        first_body,
        [shape(rank, rank), shape(8, own), shape(row_devices, own)],
        packed,
        sketch,
        targets,
        ridge,
    )
    product = kernel_times(kerns, exchanged(send, ROW))
    image, send = call(
        image_body,
        [shape(8, own), shape(everyone, 384)],
        exchanged(product, COL),
        state,
        sketch,
        targets,
        ridge,
    )
    following, send = call(
        second_body,
        [shape(8, own), shape(everyone, own)],
        exchanged(send, COL_ROW),
        state,
        image,
        inverse,
        sketch,
        targets,
        ridge,
    )
    every = exchanged(send, COL_ROW)
    product = call(last_product_body, shape(everyone, 384), *kerns, every, limit=KLIMIT2)
    coefficients, residual = call(
        finish_body,
        [shape(1, own), shape(1, own)],
        exchanged(product, COL_ROW),
        every,
        state,
        following,
        image,
        targets,
        ridge,
    )
    return coefficients.reshape(own), residual.reshape(own), sketch_out


def solution(mesh):
    split = Mesh(mesh.devices.reshape(4, 4, 4, 2), ROW + COL)

    return jax.shard_map(
        local,
        mesh=split,
        in_specs=(P(COL_ROW, None), P(), P(COL_ROW, None), P(COL_ROW), P()),
        out_specs=(P(COL_ROW), P(COL_ROW), P(COL_ROW, None)),
        check_vma=False,
    )
```

```python
import functools

import jax
import jax.numpy as jnp
from jax import lax
from jax.experimental import pallas as pl
from jax.experimental.pallas import tpu as pltpu
from jax.sharding import Mesh
from jax.sharding import PartitionSpec as P


AXES = ("row_0", "row_1", "row_2", "col_0", "col_1")
ALL = ("col_0", "col_1", "row_0", "row_1", "row_2")
NEAR_COLUMNS = ("row_0", "row_2")
COLUMNS = ("col_1", "row_0", "row_2")
ROWS = ("row_1", "col_0")
LOG2E = 1.4426950408889634
MIB = 1024 * 1024
F32 = jnp.float32
BF16 = jnp.bfloat16
HIGH = lax.Precision.HIGHEST
KERN_SPACE = pltpu.VMEM
ORDER = (2, 1, 3, 0)
KLIMIT = 4
KLIMIT2 = 4


def call(body, outs, *args, scratch=(), limit=4):
    return pl.pallas_call(
        body,
        out_shape=outs,
        scratch_shapes=list(scratch),
        compiler_params=pltpu.CompilerParams(vmem_limit_bytes=limit * MIB),
    )(*args)


def shape(*dims, dtype=F32):
    return jax.ShapeDtypeStruct(dims, dtype)


def exchanged(pieces, axes):
    return lax.all_to_all(pieces, axes, 0, 0, tiled=True)


def split3(value):
    first = value.astype(BF16)
    rest = value - first.astype(F32)
    second = rest.astype(BF16)
    third = (rest - second.astype(F32)).astype(BF16)
    return first, second, third


def parts_body(
    points_ref, scale_ref, test_ref, out_ref, copies_ref, points_scr, scale_scr, message_scr, in_sem, out_sem
):
    inputs = (
        (points_ref, points_scr),
        (scale_ref, scale_scr),
        (test_ref, message_scr.at[:, 128:384]),
    )
    loads = [pltpu.make_async_copy(*pair, in_sem.at[i]) for i, pair in enumerate(inputs)]
    for load in loads:
        load.start()
    loads[0].wait()
    loads[1].wait()
    y = points_scr[...].T * (scale_scr[...] * LOG2E**0.5)
    first = y.astype(BF16).astype(F32)
    second = (y - first).astype(BF16).astype(F32)
    parts = jnp.concatenate([first, second], axis=1).astype(BF16)
    out_ref[...] = parts
    message_scr[:, 0:128] = parts
    loads[2].wait()
    stores = [
        pltpu.make_async_copy(message_scr, copies_ref.at[i], out_sem.at[i])
        for i in range(copies_ref.shape[0])
    ]
    for store in stores:
        store.start()
    for store in stores:
        store.wait()


def parts_and_copies(points, scale, test, copies):
    own, features = points.shape
    lanes = 128 + test.shape[1]
    anywhere = pl.BlockSpec(memory_space=pltpu.HBM)
    return pl.pallas_call(
        parts_body,
        in_specs=[anywhere] * 3,
        out_specs=[pl.BlockSpec(memory_space=pltpu.VMEM), anywhere],
        out_shape=[shape(own, 128, dtype=BF16), pltpu.HBM((copies, own, lanes), BF16)],
        scratch_shapes=[
            pltpu.VMEM((features, own), F32),
            pltpu.VMEM((1, features), F32),
            pltpu.VMEM((own, lanes), BF16),
            pltpu.SemaphoreType.DMA((3,)),
            pltpu.SemaphoreType.DMA((copies,)),
        ],
        compiler_params=pltpu.CompilerParams(vmem_limit_bytes=4 * MIB),
        name="parts",
    )(*(pltpu.with_memory_space_constraint(a, pltpu.HBM) for a in (points.T, scale, test)))


def norms_body(message_ref, norm_ref):
    lane = lax.broadcasted_iota(jnp.int32, (128, 128), 1)
    sub = lax.broadcasted_iota(jnp.int32, (128, 128), 0)
    twice = jnp.where((lane - sub) % 64 == 0, 1.0, 0.0).astype(BF16)
    points = jnp.dot(message_ref[:, 0:128], twice, preferred_element_type=F32)
    squares = -0.25 * (points * points)
    lane8, sub8 = lane[0:8], sub[0:8]
    for base in range(0, message_ref.shape[0], 128):
        packed = jnp.zeros((8, 128), F32)
        for at in range(0, 128, 8):
            total = jnp.sum(squares[base + at : base + at + 8], axis=1, keepdims=True)
            packed = packed + jnp.where(lane8 == sub8 + at, total, 0.0)
        norm_ref[:, base : base + 128] = eight(jnp.sum(packed, axis=0, keepdims=True))


def block_body(*refs, chunk, has_before):
    first_ref, second_ref, message_ref, norm_ref, *rest = refs
    parts = jnp.concatenate([first_ref[...], second_ref[...]], axis=0)
    turned = pltpu.roll(parts.astype(F32), 64, 1)
    points = parts.astype(F32) + turned
    left_norm = -0.25 * jnp.sum(points * points, axis=1, keepdims=True)
    left = jnp.concatenate([parts, turned.astype(BF16)], axis=1)
    total = None
    if has_before:
        own_before_ref, other_before_ref, *rest = rest
        total = jnp.concatenate([own_before_ref[...], other_before_ref[...]], axis=0)
    kern_ref, own_ref, other_ref = rest
    for start in range(0, message_ref.shape[0], chunk):
        span = slice(start, start + chunk)
        right = message_ref[span, 0:128]
        exponent = lax.dot_general(
            left,
            jnp.concatenate([right, right], axis=1),
            (((1,), (1,)), ((), ())),
            preferred_element_type=F32,
        )
        weights = jnp.exp2(exponent + left_norm + norm_ref[0:1, span])
        kern_ref[:, span] = weights
        part = jnp.dot(
            weights.astype(BF16), message_ref[span, 128:], preferred_element_type=F32
        )
        total = part if total is None else total + part
    half = total.shape[0] // 2
    own_ref[...] = total[:half]
    other_ref[...] = total[half:]


def kernel_block(first, second, message, norm, before=()):
    rows, columns, rank = first.shape[0], message.shape[0], message.shape[1] - 128
    return call(
        functools.partial(block_body, chunk=512, has_before=bool(before)),
        [KERN_SPACE((2 * rows, columns), F32), shape(rows, rank), shape(rows, rank)],
        first,
        second,
        message,
        norm,
        *before,
        limit=KLIMIT,
    )


def core_body(
    *refs
):
    *part_refs, test_ref, targets_ref, ridge_ref, sketch_ref, copy_ref, out_ref = refs
    sketch = part_refs[0][...]
    for part_ref in part_refs[1:]:
        sketch = sketch + part_ref[...]
    sketch_ref[...] = sketch
    copy_ref[...] = sketch
    shifted = ridge_ref[0, 0] * test_ref[...].astype(F32) + sketch
    core = lax.dot_general(
        shifted, sketch, (((0,), (0,)), ((), ())), precision=HIGH, preferred_element_type=F32
    )
    targets = jnp.broadcast_to(targets_ref[...], (8, 256))
    projected = jnp.dot(targets, sketch, precision=HIGH, preferred_element_type=F32)
    square = jnp.sum(targets[0:1] * targets[0:1], axis=1, keepdims=True)
    row = lax.broadcasted_iota(jnp.int32, (8, 128), 0)
    extra = jnp.where(row == 2, square, 0.0)
    extra = jnp.where(row == 1, projected[:, 128:256], extra)
    extra = jnp.where(row == 0, projected[:, 0:128], extra)
    out_ref[:, 0:256] = core[0:128]
    out_ref[:, 256:384] = core[128:256, 128:256]
    out_ref[:, 384:512] = jnp.zeros((128, 128), F32)
    out_ref[0:8, 384:512] = extra


def summed_body(parts_ref, out_ref):
    out_ref[...] = jnp.broadcast_to(jnp.sum(parts_ref[...], axis=0, keepdims=True), out_ref.shape)


def inverted(work_ref):
    size = work_ref.shape[0]
    panels = size // 8
    sub = lax.broadcasted_iota(jnp.int32, (8, 1), 0)
    lanes = lax.broadcasted_iota(jnp.int32, (1, size), 1)

    def column(block, step, j):
        index = jnp.full((8, 128), 0, jnp.int32) + ((step % 16) * 8 + j)
        window = jnp.where(step < 16, block[:, 0:128], block[:, 128:256])
        return jnp.take_along_axis(window, index, axis=1)

    def wide(value):
        return jnp.concatenate([value, value], axis=1)

    def eliminated(panel, step):
        diag = [column(panel, step, j) for j in range(8)]
        for j in range(0, 8, 2):
            a, b = diag[j][j : j + 1, :], diag[j + 1][j : j + 1, :]
            c, d = diag[j][j + 1 : j + 2, :], diag[j + 1][j + 1 : j + 2, :]
            inverse = 1.0 / (a * d - b * c)
            upper, lower = sub == j, sub == j + 1

            def swept(block, first, second, spread=lambda value: value):
                top, bottom = block[j : j + 1, :], block[j + 1 : j + 2, :]
                new_top = (spread(d) * top - spread(b) * bottom) * spread(inverse)
                new_bottom = (spread(a) * bottom - spread(c) * top) * spread(inverse)
                rest = block - first * new_top - second * new_bottom
                return jnp.where(upper, new_top, jnp.where(lower, new_bottom, rest))

            for k in range(j + 2, 8):
                diag[k] = swept(diag[k], diag[j], diag[j + 1])
            panel = jnp.where(lanes == step * 8 + j, jnp.where(upper, 1.0, 0.0), panel)
            panel = jnp.where(lanes == step * 8 + j + 1, jnp.where(lower, 1.0, 0.0), panel)
            panel = swept(panel, wide(diag[j]), wide(diag[j + 1]), wide)
        return panel

    def split(value):
        return [part.astype(F32) for part in split3(value)]

    def stacked(parts):
        return jnp.concatenate(parts, axis=0).astype(BF16)

    def panel_step(step, carry):
        panel, factors = carry
        following = jnp.minimum(step + 1, panels - 1)
        here = pl.ds(pl.multiple_of(step * 8, 8), 8)
        ahead = work_ref[pl.ds(pl.multiple_of(following * 8, 8), 8), :]
        inside = (lanes >= step * 8) & (lanes < step * 8 + 8)
        following_rows = jnp.where(inside, 0.0, ahead)
        for j in range(8):
            following_rows = following_rows - wide(column(ahead, step, j)) * panel[j : j + 1, :]
        f1, f2, f3 = split(factors)
        p1, p2, p3 = split(panel)
        update = lax.dot_general(
            stacked([f1, f1, f2, f2, f1, f3]),
            stacked([p1, p2, p1, p2, p3, p1]),
            (((0,), (0,)), ((), ())),
            preferred_element_type=F32,
        )
        work_ref[...] = jnp.where(inside, 0.0, work_ref[...]) - update
        work_ref[here, :] = panel
        following_factors = jnp.where(lanes < following * 8, -following_rows, following_rows)
        return eliminated(following_rows, following), following_factors

    start = work_ref[0:8, :]
    lax.fori_loop(0, panels, panel_step, (eliminated(start, 0), start))


def eight(row):
    return jnp.broadcast_to(row, (8, row.shape[1]))


def row_dot(a, b):
    return jnp.sum(a * b, axis=1, keepdims=True)


def times(vector, matrix, transposed=False):
    dims = (((1,), (1 if transposed else 0,)), ((), ()))
    return lax.dot_general(vector, matrix, dims, precision=HIGH, preferred_element_type=F32)


def first_body(packed_ref, sketch_ref, targets_ref, ridge_ref, inverse_ref, state_ref, send_ref):
    inverse_ref[0:128, :] = packed_ref[:, 0:256]
    inverse_ref[128:256, 0:128] = packed_ref[:, 128:256].T
    inverse_ref[128:256, 128:256] = packed_ref[:, 256:384]
    inverted(inverse_ref)
    projected = jnp.concatenate([packed_ref[0:1, 384:512], packed_ref[1:2, 384:512]], axis=1)
    square = packed_ref[2:3, 384:385]
    solved = times(eight(projected), inverse_ref[...])
    fitted = times(solved, sketch_ref[...], transposed=True)
    ridge = ridge_ref[0, 0]
    direction = (targets_ref[...] - fitted[0:1]) / ridge
    descent = (square - row_dot(projected, solved[0:1])) / ridge
    state_ref[0:1, :] = direction
    state_ref[1:2, :] = projected
    state_ref[2:3, :] = jnp.broadcast_to(square, (1, 256))
    state_ref[3:4, :] = jnp.broadcast_to(descent, (1, 256))
    send_ref[...] = jnp.broadcast_to(direction, send_ref.shape)


def products(kern_refs, vector):
    sub = lax.broadcasted_iota(jnp.int32, (8, 128), 0)
    lane = lax.broadcasted_iota(jnp.int32, (8, 128), 1)
    chips = len(ORDER)
    tiles = kern_refs[0].shape[1] // 128
    for number, shift in enumerate(ORDER):
        pair = (kern_refs[number], kern_refs[number + chips])
        for half in range(2):
            pieces = []
            for flip in range(2):
                packed = jnp.zeros((8, 128), F32)
                for start in range(0, 128, 64):
                    base = flip * 256 + half * 128 + start
                    acc = [None] * 8
                    for k in range(2 * tiles):
                        span = slice(k % 2 * 128, k % 2 * 128 + 128)
                        piece = eight(vector[k // 2 : k // 2 + 1, span])
                        at = k % tiles * 128
                        for g in range(8):
                            block = pair[k // tiles][
                                base + g * 8 : base + g * 8 + 8, at : at + 128
                            ]
                            acc[g] = block * piece if k == 0 else acc[g] + block * piece
                    for g in range(8):
                        total = jnp.sum(acc[g], axis=1, keepdims=True)
                        packed = packed + jnp.where(lane == sub + (start + g * 8), total, 0.0)
                pieces.append(jnp.sum(packed, axis=0, keepdims=True))
            yield shift, half, pieces


def own_first(lower, upper):
    core = lax.axis_index("col_1")
    return jnp.concatenate(
        [jnp.where(core == 0, lower, upper), jnp.where(core == 0, upper, lower)], axis=0
    )


def owner(shift):
    chips = len(ORDER)
    return (lax.axis_index("col_0") + (chips - shift)) % chips


def product_body(*refs):
    *kern_refs, vector_ref, out_ref = refs
    half_y = lax.axis_index("row_1")
    chips = len(ORDER)
    vector = own_first(vector_ref[0:8, :], vector_ref[8:16, :])
    for shift, half, pieces in products(kern_refs, vector):
        span = slice(half * 128, half * 128 + 128)
        out_ref[half_y * chips + owner(shift), :, span] = eight(pieces[0])
        out_ref[(1 - half_y) * chips + owner(shift), :, span] = eight(pieces[1])


def last_product_body(*refs):
    *kern_refs, vector_ref, out_ref = refs
    chip, core = lax.axis_index("col_0"), lax.axis_index("col_1")
    far_y, half_y, z = lax.axis_index("row_0"), lax.axis_index("row_1"), lax.axis_index("row_2")

    def group(chip, core, far_y):
        return pl.ds(pl.multiple_of(chip * 32 + core * 16 + far_y * 8, 8), 8)

    def columns_of(core):
        rows = [vector_ref[group(chip, core, far), :] for far in range(2)]
        return jnp.concatenate(
            [jnp.where(half_y == 0, block[0:4], block[4:8]) for block in rows], axis=0
        )

    sub = lax.broadcasted_iota(jnp.int32, (8, 128), 0)
    mine = sub // 4 == half_y
    curve = jnp.zeros((8, 128), F32)
    out_ref[...] = jnp.zeros(out_ref.shape, F32)
    vector = own_first(columns_of(0), columns_of(1))
    for shift, half, pieces in products(kern_refs, vector):
        span = slice(half * 128, half * 128 + 128)
        rows = group(owner(shift), core, far_y)
        both = jnp.where(mine, pieces[0], pieces[1])
        out_ref[rows, span] = both
        curve = curve + jnp.where(sub % 4 == z, both * vector_ref[rows, span], 0.0)
    curve = jnp.sum(curve, axis=0, keepdims=True)
    out_ref[:, 256:384] = jnp.broadcast_to(curve, (out_ref.shape[0], 128))


def kernel_times(kerns, vector):
    return call(product_body, shape(8, 8, 256), *kerns, vector, limit=KLIMIT2)


def image_body(parts_ref, state_ref, sketch_ref, targets_ref, ridge_ref, image_ref, send_ref):
    image = jnp.sum(parts_ref[...], axis=0)[0:1] + ridge_ref[0, 0] * state_ref[0:1, :]
    image_ref[...] = eight(image)
    along = times(eight(image), sketch_ref[...])[0:1]
    lane = lax.broadcasted_iota(jnp.int32, (1, 128), 1)
    sums = jnp.where(
        lane == 0,
        row_dot(state_ref[0:1, :], image),
        jnp.where(
            lane == 1, row_dot(image, image), jnp.where(lane == 2, row_dot(targets_ref[...], image), 0.0)
        ),
    )
    send_ref[:, 0:256] = jnp.broadcast_to(along, (send_ref.shape[0], 256))
    send_ref[:, 256:384] = jnp.broadcast_to(sums, (send_ref.shape[0], 128))


def second_body(
    parts_ref, state_ref, image_ref, inverse_ref, sketch_ref, targets_ref, ridge_ref, next_ref, send_ref
):
    sums = jnp.sum(parts_ref[...], axis=0, keepdims=True)
    along = sums[:, 0:256]
    curve, image_square, cross = sums[:, 256:257], sums[:, 257:258], sums[:, 258:259]
    ridge = ridge_ref[0, 0]
    descent = state_ref[3:4, :]
    step = descent / curve
    projected = state_ref[1:2, :] - step * along
    solved = times(eight(projected), inverse_ref[...])
    fitted = times(solved, sketch_ref[...], transposed=True)[0:1]
    resid = targets_ref[...] - step * image_ref[0:1, :]
    square = state_ref[2:3, :] - 2.0 * step * cross + step * step * image_square
    fresh = (square - row_dot(projected, solved[0:1])) / ridge
    direction = (resid - fitted) / ridge + fresh / descent * state_ref[0:1, :]
    next_ref[0:1, :] = direction
    next_ref[1:2, :] = step
    next_ref[2:3, :] = fresh
    send_ref[...] = jnp.broadcast_to(direction, send_ref.shape)


def finish_body(
    parts_ref,
    every_ref,
    state_ref,
    next_ref,
    image_ref,
    targets_ref,
    ridge_ref,
    coefficients_ref,
    residual_ref,
):
    ridge = ridge_ref[0, 0]
    group = lax.axis_index("col_1") * 2 + lax.axis_index("row_0")
    direction = next_ref[0:1, :]
    row = lax.broadcasted_iota(jnp.int32, (parts_ref.shape[0], 256), 0)
    mine = (row % 32 // 8 == group) & (row % 4 == lax.axis_index("row_2"))
    last = jnp.sum(jnp.where(mine, parts_ref[:, 0:256], 0.0), axis=0, keepdims=True)
    last = last + ridge * direction
    every = every_ref[...]
    square = jnp.sum(jnp.sum(every * every, axis=0, keepdims=True), axis=1, keepdims=True)
    curve = jnp.sum(
        jnp.sum(parts_ref[:, 256:384], axis=0, keepdims=True), axis=1, keepdims=True
    )
    step = next_ref[1:2, :]
    last_step = next_ref[2:3, :] / (curve + ridge * square)
    coefficients_ref[...] = step * state_ref[0:1, :] + last_step * direction
    residual_ref[...] = targets_ref[...] - step * image_ref[0:1, :] - last_step * last


def local(points, feature_scale, test_matrix, targets, ridge):
    everyone = lax.axis_size(ALL)
    column_devices, near_devices = lax.axis_size(COLUMNS), lax.axis_size(NEAR_COLUMNS)
    own, rank = test_matrix.shape
    ridge = ridge.reshape(1, 1)
    targets = targets.reshape(1, own)
    scale = feature_scale.reshape(1, -1)
    parts, copies = parts_and_copies(points, scale, test_matrix, near_devices)
    chips = lax.axis_size("col_0")

    def along_rows(value, shift, flip):
        pairs = [
            (i, (i // chips ^ flip) * chips + (i + shift) % chips) for i in range(2 * chips)
        ]
        return lax.ppermute(value, ROWS, pairs) if shift or flip else value

    chunks = {
        (shift, flip): along_rows(parts, shift, flip) for shift in ORDER for flip in (0, 1)
    }
    message = exchanged(copies, NEAR_COLUMNS).reshape(-1, 128 + rank)
    message, chunks = lax.optimization_barrier((message, chunks))
    partner = lax.ppermute(message, "col_1", [(0, 1), (1, 0)])
    norm = call(norms_body, shape(8, message.shape[0]), message)
    kerns, before, sums = [], [], []
    for shift in ORDER:
        kern, *sketches = kernel_block(chunks[shift, 0], chunks[shift, 1], message, norm)
        kerns.append(kern)
        before.append(sketches)
    norm = call(norms_body, shape(8, message.shape[0]), partner)
    for number, shift in enumerate(ORDER):
        kern, *sketches = kernel_block(
            chunks[shift, 0], chunks[shift, 1], partner, norm, before[number]
        )
        kerns.append(kern)
        for flip in (1, 0):
            sums.append(along_rows(sketches[flip], -shift, flip))
    sketch_out, sketch, packed = call(
        core_body,
        [shape(own, rank), shape(own, rank), shape(everyone, 512)],
        *sums,
        test_matrix,
        targets,
        ridge,
    )
    packed = exchanged(packed, ALL)
    packed = call(summed_body, shape(everyone, 512), packed)
    packed = exchanged(packed, ALL)
    inverse, state, send = call(
        first_body,
        [shape(rank, rank), shape(8, own), shape(column_devices, own)],
        packed,
        sketch,
        targets,
        ridge,
    )
    product = kernel_times(kerns, exchanged(send, COLUMNS))
    image, send = call(
        image_body,
        [shape(8, own), shape(everyone, 384)],
        exchanged(product, ROWS),
        state,
        sketch,
        targets,
        ridge,
    )
    following, send = call(
        second_body,
        [shape(8, own), shape(everyone, own)],
        exchanged(send, ALL),
        state,
        image,
        inverse,
        sketch,
        targets,
        ridge,
    )
    every = exchanged(send, ALL)
    product = call(last_product_body, shape(everyone, 384), *kerns, every, limit=KLIMIT2)
    coefficients, residual = call(
        finish_body,
        [shape(1, own), shape(1, own)],
        exchanged(product, ALL),
        every,
        state,
        following,
        image,
        targets,
        ridge,
    )
    return coefficients.reshape(own), residual.reshape(own), sketch_out


def solution(mesh):
    split = Mesh(mesh.devices.reshape(2, 2, 4, 4, 2), AXES)

    return jax.shard_map(
        local,
        mesh=split,
        in_specs=(P(ALL, None), P(), P(ALL, None), P(ALL), P()),
        out_specs=(P(ALL), P(ALL), P(ALL, None)),
        check_vma=False,
    )
```

```python
import functools

import jax
import jax.numpy as jnp
from jax import lax
from jax.experimental import pallas as pl
from jax.experimental.pallas import tpu as pltpu
from jax.sharding import Mesh
from jax.sharding import PartitionSpec as P


AXES = ("row_0", "row_1", "row_2", "col_0", "col_1")
ALL = ("col_0", "col_1", "row_0", "row_1", "row_2")
NEAR_COLUMNS = ("row_0", "row_2")
COLUMNS = ("col_1", "row_0", "row_2")
ROWS = ("row_1", "col_0")
LOG2E = 1.4426950408889634
MIB = 1024 * 1024
WIDTH = 16
F32 = jnp.float32
BF16 = jnp.bfloat16
HIGH = lax.Precision.HIGHEST
KERN_SPACE = pltpu.VMEM
ORDER = (2, 1, 3, 0)
KLIMIT = 4
KLIMIT2 = 4


def call(body, outs, *args, scratch=(), limit=4):
    return pl.pallas_call(
        body,
        out_shape=outs,
        scratch_shapes=list(scratch),
        compiler_params=pltpu.CompilerParams(vmem_limit_bytes=limit * MIB),
    )(*args)


def shape(*dims, dtype=F32):
    return jax.ShapeDtypeStruct(dims, dtype)


def exchanged(pieces, axes):
    return lax.all_to_all(pieces, axes, 0, 0, tiled=True)


def split3(value):
    first = value.astype(BF16)
    rest = value - first.astype(F32)
    second = rest.astype(BF16)
    third = (rest - second.astype(F32)).astype(BF16)
    return first, second, third


def parts_body(
    points_ref, scale_ref, test_ref, out_ref, copies_ref, points_scr, scale_scr, message_scr, in_sem, out_sem
):
    inputs = (
        (points_ref, points_scr),
        (scale_ref, scale_scr),
        (test_ref, message_scr.at[:, 128:384]),
    )
    loads = [pltpu.make_async_copy(*pair, in_sem.at[i]) for i, pair in enumerate(inputs)]
    for load in loads:
        load.start()
    loads[0].wait()
    loads[1].wait()
    y = points_scr[...].T * (scale_scr[...] * LOG2E**0.5)
    first = y.astype(BF16).astype(F32)
    second = (y - first).astype(BF16).astype(F32)
    parts = jnp.concatenate([first, second], axis=1).astype(BF16)
    out_ref[...] = parts
    message_scr[:, 0:128] = parts
    loads[2].wait()
    stores = [
        pltpu.make_async_copy(message_scr, copies_ref.at[i], out_sem.at[i])
        for i in range(copies_ref.shape[0])
    ]
    for store in stores:
        store.start()
    for store in stores:
        store.wait()


def parts_and_copies(points, scale, test, copies):
    own, features = points.shape
    lanes = 128 + test.shape[1]
    anywhere = pl.BlockSpec(memory_space=pltpu.HBM)
    return pl.pallas_call(
        parts_body,
        in_specs=[anywhere] * 3,
        out_specs=[pl.BlockSpec(memory_space=pltpu.VMEM), anywhere],
        out_shape=[shape(own, 128, dtype=BF16), pltpu.HBM((copies, own, lanes), BF16)],
        scratch_shapes=[
            pltpu.VMEM((features, own), F32),
            pltpu.VMEM((1, features), F32),
            pltpu.VMEM((own, lanes), BF16),
            pltpu.SemaphoreType.DMA((3,)),
            pltpu.SemaphoreType.DMA((copies,)),
        ],
        compiler_params=pltpu.CompilerParams(vmem_limit_bytes=4 * MIB),
        name="parts",
    )(*(pltpu.with_memory_space_constraint(a, pltpu.HBM) for a in (points.T, scale, test)))


def norms_body(message_ref, norm_ref):
    lane = lax.broadcasted_iota(jnp.int32, (128, 128), 1)
    sub = lax.broadcasted_iota(jnp.int32, (128, 128), 0)
    twice = jnp.where((lane - sub) % 64 == 0, 1.0, 0.0).astype(BF16)
    points = jnp.dot(message_ref[:, 0:128], twice, preferred_element_type=F32)
    squares = -0.25 * (points * points)
    lane8, sub8 = lane[0:8], sub[0:8]
    for base in range(0, message_ref.shape[0], 128):
        packed = jnp.zeros((8, 128), F32)
        for at in range(0, 128, 8):
            total = jnp.sum(squares[base + at : base + at + 8], axis=1, keepdims=True)
            packed = packed + jnp.where(lane8 == sub8 + at, total, 0.0)
        norm_ref[:, base : base + 128] = eight(jnp.sum(packed, axis=0, keepdims=True))


def block_body(*refs, chunk, has_before):
    first_ref, second_ref, message_ref, norm_ref, *rest = refs
    parts = jnp.concatenate([first_ref[...], second_ref[...]], axis=0)
    turned = pltpu.roll(parts.astype(F32), 64, 1)
    points = parts.astype(F32) + turned
    left_norm = -0.25 * jnp.sum(points * points, axis=1, keepdims=True)
    left = jnp.concatenate([parts, turned.astype(BF16)], axis=1)
    total = None
    if has_before:
        own_before_ref, other_before_ref, *rest = rest
        total = jnp.concatenate([own_before_ref[...], other_before_ref[...]], axis=0)
    kern_ref, own_ref, other_ref = rest
    for start in range(0, message_ref.shape[0], chunk):
        span = slice(start, start + chunk)
        right = message_ref[span, 0:128]
        exponent = lax.dot_general(
            left,
            jnp.concatenate([right, right], axis=1),
            (((1,), (1,)), ((), ())),
            preferred_element_type=F32,
        )
        weights = jnp.exp2(exponent + left_norm + norm_ref[0:1, span])
        kern_ref[:, span] = weights
        part = jnp.dot(
            weights.astype(BF16), message_ref[span, 128:], preferred_element_type=F32
        )
        total = part if total is None else total + part
    half = total.shape[0] // 2
    own_ref[...] = total[:half]
    other_ref[...] = total[half:]


def kernel_block(first, second, message, norm, before=()):
    rows, columns, rank = first.shape[0], message.shape[0], message.shape[1] - 128
    return call(
        functools.partial(block_body, chunk=512, has_before=bool(before)),
        [KERN_SPACE((2 * rows, columns), F32), shape(rows, rank), shape(rows, rank)],
        first,
        second,
        message,
        norm,
        *before,
        limit=KLIMIT,
    )


def core_body(
    *refs
):
    *part_refs, test_ref, targets_ref, ridge_ref, sketch_ref, copy_ref, out_ref = refs
    sketch = part_refs[0][...]
    for part_ref in part_refs[1:]:
        sketch = sketch + part_ref[...]
    sketch_ref[...] = sketch
    copy_ref[...] = sketch
    shifted = ridge_ref[0, 0] * test_ref[...].astype(F32) + sketch
    core = lax.dot_general(
        shifted, sketch, (((0,), (0,)), ((), ())), precision=HIGH, preferred_element_type=F32
    )
    targets = jnp.broadcast_to(targets_ref[...], (8, 256))
    projected = jnp.dot(targets, sketch, precision=HIGH, preferred_element_type=F32)
    square = jnp.sum(targets[0:1] * targets[0:1], axis=1, keepdims=True)
    row = lax.broadcasted_iota(jnp.int32, (8, 128), 0)
    extra = jnp.where(row == 2, square, 0.0)
    extra = jnp.where(row == 1, projected[:, 128:256], extra)
    extra = jnp.where(row == 0, projected[:, 0:128], extra)
    out_ref[:, 0:256] = core[0:128]
    out_ref[:, 256:384] = core[128:256, 128:256]
    out_ref[:, 384:512] = jnp.zeros((128, 128), F32)
    out_ref[0:8, 384:512] = extra


def summed_body(parts_ref, out_ref):
    out_ref[...] = jnp.broadcast_to(jnp.sum(parts_ref[...], axis=0, keepdims=True), out_ref.shape)


def inverted(work_ref):
    size = work_ref.shape[0]
    panels = size // WIDTH
    per_window = 128 // WIDTH
    sub = lax.broadcasted_iota(jnp.int32, (WIDTH, 1), 0)
    lanes = lax.broadcasted_iota(jnp.int32, (1, size), 1)

    def column(block, step, j):
        index = jnp.full((WIDTH, 128), 0, jnp.int32) + ((step % per_window) * WIDTH + j)
        window = jnp.where(step < per_window, block[:, 0:128], block[:, 128:256])
        return jnp.take_along_axis(window, index, axis=1)

    def wide(value):
        return jnp.concatenate([value, value], axis=1)

    def eliminated(panel, step):
        diag = [column(panel, step, j) for j in range(WIDTH)]
        for j in range(0, WIDTH, 2):
            a, b = diag[j][j : j + 1, :], diag[j + 1][j : j + 1, :]
            c, d = diag[j][j + 1 : j + 2, :], diag[j + 1][j + 1 : j + 2, :]
            inverse = 1.0 / (a * d - b * c)
            upper, lower = sub == j, sub == j + 1

            def swept(block, first, second, spread=lambda value: value):
                top, bottom = block[j : j + 1, :], block[j + 1 : j + 2, :]
                new_top = (spread(d) * top - spread(b) * bottom) * spread(inverse)
                new_bottom = (spread(a) * bottom - spread(c) * top) * spread(inverse)
                rest = block - first * new_top - second * new_bottom
                return jnp.where(upper, new_top, jnp.where(lower, new_bottom, rest))

            for k in range(j + 2, WIDTH):
                diag[k] = swept(diag[k], diag[j], diag[j + 1])
            panel = jnp.where(lanes == step * WIDTH + j, jnp.where(upper, 1.0, 0.0), panel)
            panel = jnp.where(lanes == step * WIDTH + j + 1, jnp.where(lower, 1.0, 0.0), panel)
            panel = swept(panel, wide(diag[j]), wide(diag[j + 1]), wide)
        return panel

    def split(value):
        return [part.astype(F32) for part in split3(value)]

    def stacked(parts):
        return jnp.concatenate(parts, axis=0).astype(BF16)

    def panel_step(step, carry):
        panel, factors = carry
        following = jnp.minimum(step + 1, panels - 1)
        here = pl.ds(pl.multiple_of(step * WIDTH, WIDTH), WIDTH)
        ahead = work_ref[pl.ds(pl.multiple_of(following * WIDTH, WIDTH), WIDTH), :]
        inside = (lanes >= step * WIDTH) & (lanes < step * WIDTH + WIDTH)
        following_rows = jnp.where(inside, 0.0, ahead)
        for j in range(WIDTH):
            following_rows = following_rows - wide(column(ahead, step, j)) * panel[j : j + 1, :]
        f1, f2, f3 = split(factors)
        p1, p2, p3 = split(panel)
        update = lax.dot_general(
            stacked([f1, f1, f2, f2, f1, f3]),
            stacked([p1, p2, p1, p2, p3, p1]),
            (((0,), (0,)), ((), ())),
            preferred_element_type=F32,
        )
        work_ref[...] = jnp.where(inside, 0.0, work_ref[...]) - update
        work_ref[here, :] = panel
        following_factors = jnp.where(lanes < following * WIDTH, -following_rows, following_rows)
        return eliminated(following_rows, following), following_factors

    start = work_ref[0:WIDTH, :]
    lax.fori_loop(0, panels, panel_step, (eliminated(start, 0), start))


def eight(row):
    return jnp.broadcast_to(row, (8, row.shape[1]))


def row_dot(a, b):
    return jnp.sum(a * b, axis=1, keepdims=True)


def times(vector, matrix, transposed=False):
    dims = (((1,), (1 if transposed else 0,)), ((), ()))
    return lax.dot_general(vector, matrix, dims, precision=HIGH, preferred_element_type=F32)


def first_body(packed_ref, sketch_ref, targets_ref, ridge_ref, inverse_ref, state_ref, send_ref):
    inverse_ref[0:128, :] = packed_ref[:, 0:256]
    inverse_ref[128:256, 0:128] = packed_ref[:, 128:256].T
    inverse_ref[128:256, 128:256] = packed_ref[:, 256:384]
    inverted(inverse_ref)
    projected = jnp.concatenate([packed_ref[0:1, 384:512], packed_ref[1:2, 384:512]], axis=1)
    square = packed_ref[2:3, 384:385]
    solved = times(eight(projected), inverse_ref[...])
    fitted = times(solved, sketch_ref[...], transposed=True)
    ridge = ridge_ref[0, 0]
    direction = (targets_ref[...] - fitted[0:1]) / ridge
    descent = (square - row_dot(projected, solved[0:1])) / ridge
    state_ref[0:1, :] = direction
    state_ref[1:2, :] = projected
    state_ref[2:3, :] = jnp.broadcast_to(square, (1, 256))
    state_ref[3:4, :] = jnp.broadcast_to(descent, (1, 256))
    send_ref[...] = jnp.broadcast_to(direction, send_ref.shape)


def products(kern_refs, vector):
    sub = lax.broadcasted_iota(jnp.int32, (8, 128), 0)
    lane = lax.broadcasted_iota(jnp.int32, (8, 128), 1)
    chips = len(ORDER)
    tiles = kern_refs[0].shape[1] // 128
    for number, shift in enumerate(ORDER):
        pair = (kern_refs[number], kern_refs[number + chips])
        for half in range(2):
            pieces = []
            for flip in range(2):
                packed = jnp.zeros((8, 128), F32)
                for start in range(0, 128, 64):
                    base = flip * 256 + half * 128 + start
                    acc = [None] * 8
                    for k in range(2 * tiles):
                        span = slice(k % 2 * 128, k % 2 * 128 + 128)
                        piece = eight(vector[k // 2 : k // 2 + 1, span])
                        at = k % tiles * 128
                        for g in range(8):
                            block = pair[k // tiles][
                                base + g * 8 : base + g * 8 + 8, at : at + 128
                            ]
                            acc[g] = block * piece if k == 0 else acc[g] + block * piece
                    for g in range(8):
                        total = jnp.sum(acc[g], axis=1, keepdims=True)
                        packed = packed + jnp.where(lane == sub + (start + g * 8), total, 0.0)
                pieces.append(jnp.sum(packed, axis=0, keepdims=True))
            yield shift, half, pieces


def own_first(lower, upper):
    core = lax.axis_index("col_1")
    return jnp.concatenate(
        [jnp.where(core == 0, lower, upper), jnp.where(core == 0, upper, lower)], axis=0
    )


def owner(shift):
    chips = len(ORDER)
    return (lax.axis_index("col_0") + (chips - shift)) % chips


def product_body(*refs):
    *kern_refs, vector_ref, out_ref = refs
    half_y = lax.axis_index("row_1")
    chips = len(ORDER)
    vector = own_first(vector_ref[0:8, :], vector_ref[8:16, :])
    for shift, half, pieces in products(kern_refs, vector):
        span = slice(half * 128, half * 128 + 128)
        out_ref[half_y * chips + owner(shift), :, span] = eight(pieces[0])
        out_ref[(1 - half_y) * chips + owner(shift), :, span] = eight(pieces[1])


def last_product_body(*refs):
    *kern_refs, vector_ref, out_ref = refs
    chip, core = lax.axis_index("col_0"), lax.axis_index("col_1")
    far_y, half_y, z = lax.axis_index("row_0"), lax.axis_index("row_1"), lax.axis_index("row_2")

    def group(chip, core, far_y):
        return pl.ds(pl.multiple_of(chip * 32 + core * 16 + far_y * 8, 8), 8)

    def columns_of(core):
        rows = [vector_ref[group(chip, core, far), :] for far in range(2)]
        return jnp.concatenate(
            [jnp.where(half_y == 0, block[0:4], block[4:8]) for block in rows], axis=0
        )

    sub = lax.broadcasted_iota(jnp.int32, (8, 128), 0)
    mine = sub // 4 == half_y
    curve = jnp.zeros((8, 128), F32)
    out_ref[...] = jnp.zeros(out_ref.shape, F32)
    vector = own_first(columns_of(0), columns_of(1))
    for shift, half, pieces in products(kern_refs, vector):
        span = slice(half * 128, half * 128 + 128)
        rows = group(owner(shift), core, far_y)
        both = jnp.where(mine, pieces[0], pieces[1])
        out_ref[rows, span] = both
        curve = curve + jnp.where(sub % 4 == z, both * vector_ref[rows, span], 0.0)
    curve = jnp.sum(curve, axis=0, keepdims=True)
    out_ref[:, 256:384] = jnp.broadcast_to(curve, (out_ref.shape[0], 128))


def kernel_times(kerns, vector):
    return call(product_body, shape(8, 8, 256), *kerns, vector, limit=KLIMIT2)


def image_body(parts_ref, state_ref, sketch_ref, targets_ref, ridge_ref, image_ref, send_ref):
    image = jnp.sum(parts_ref[...], axis=0)[0:1] + ridge_ref[0, 0] * state_ref[0:1, :]
    image_ref[...] = eight(image)
    along = times(eight(image), sketch_ref[...])[0:1]
    lane = lax.broadcasted_iota(jnp.int32, (1, 128), 1)
    sums = jnp.where(
        lane == 0,
        row_dot(state_ref[0:1, :], image),
        jnp.where(
            lane == 1, row_dot(image, image), jnp.where(lane == 2, row_dot(targets_ref[...], image), 0.0)
        ),
    )
    send_ref[:, 0:256] = jnp.broadcast_to(along, (send_ref.shape[0], 256))
    send_ref[:, 256:384] = jnp.broadcast_to(sums, (send_ref.shape[0], 128))


def second_body(
    parts_ref, state_ref, image_ref, inverse_ref, sketch_ref, targets_ref, ridge_ref, next_ref, send_ref
):
    sums = jnp.sum(parts_ref[...], axis=0, keepdims=True)
    along = sums[:, 0:256]
    curve, image_square, cross = sums[:, 256:257], sums[:, 257:258], sums[:, 258:259]
    ridge = ridge_ref[0, 0]
    descent = state_ref[3:4, :]
    step = descent / curve
    projected = state_ref[1:2, :] - step * along
    solved = times(eight(projected), inverse_ref[...])
    fitted = times(solved, sketch_ref[...], transposed=True)[0:1]
    resid = targets_ref[...] - step * image_ref[0:1, :]
    square = state_ref[2:3, :] - 2.0 * step * cross + step * step * image_square
    fresh = (square - row_dot(projected, solved[0:1])) / ridge
    direction = (resid - fitted) / ridge + fresh / descent * state_ref[0:1, :]
    next_ref[0:1, :] = direction
    next_ref[1:2, :] = step
    next_ref[2:3, :] = fresh
    send_ref[...] = jnp.broadcast_to(direction, send_ref.shape)


def finish_body(
    parts_ref,
    every_ref,
    state_ref,
    next_ref,
    image_ref,
    targets_ref,
    ridge_ref,
    coefficients_ref,
    residual_ref,
):
    ridge = ridge_ref[0, 0]
    group = lax.axis_index("col_1") * 2 + lax.axis_index("row_0")
    direction = next_ref[0:1, :]
    row = lax.broadcasted_iota(jnp.int32, (parts_ref.shape[0], 256), 0)
    mine = (row % 32 // 8 == group) & (row % 4 == lax.axis_index("row_2"))
    last = jnp.sum(jnp.where(mine, parts_ref[:, 0:256], 0.0), axis=0, keepdims=True)
    last = last + ridge * direction
    every = every_ref[...]
    square = jnp.sum(jnp.sum(every * every, axis=0, keepdims=True), axis=1, keepdims=True)
    curve = jnp.sum(
        jnp.sum(parts_ref[:, 256:384], axis=0, keepdims=True), axis=1, keepdims=True
    )
    step = next_ref[1:2, :]
    last_step = next_ref[2:3, :] / (curve + ridge * square)
    coefficients_ref[...] = step * state_ref[0:1, :] + last_step * direction
    residual_ref[...] = targets_ref[...] - step * image_ref[0:1, :] - last_step * last


def local(points, feature_scale, test_matrix, targets, ridge):
    everyone = lax.axis_size(ALL)
    column_devices, near_devices = lax.axis_size(COLUMNS), lax.axis_size(NEAR_COLUMNS)
    own, rank = test_matrix.shape
    ridge = ridge.reshape(1, 1)
    targets = targets.reshape(1, own)
    scale = feature_scale.reshape(1, -1)
    parts, copies = parts_and_copies(points, scale, test_matrix, near_devices)
    chips = lax.axis_size("col_0")

    def along_rows(value, shift, flip):
        pairs = [
            (i, (i // chips ^ flip) * chips + (i + shift) % chips) for i in range(2 * chips)
        ]
        return lax.ppermute(value, ROWS, pairs) if shift or flip else value

    chunks = {
        (shift, flip): along_rows(parts, shift, flip) for shift in ORDER for flip in (0, 1)
    }
    message = exchanged(copies, NEAR_COLUMNS).reshape(-1, 128 + rank)
    message, chunks = lax.optimization_barrier((message, chunks))
    partner = lax.ppermute(message, "col_1", [(0, 1), (1, 0)])
    norm = call(norms_body, shape(8, message.shape[0]), message)
    kerns, before, sums = {}, {}, []

    def near_block(number):
        shift = ORDER[number]
        kerns[number], *before[number] = kernel_block(
            chunks[shift, 0], chunks[shift, 1], message, norm
        )

    for number in range(3):
        near_block(number)
    other_norm = call(norms_body, shape(8, message.shape[0]), partner)
    for number, shift in enumerate(ORDER):
        if number == 3:
            near_block(number)
        kerns[number + 4], *sketches = kernel_block(
            chunks[shift, 0], chunks[shift, 1], partner, other_norm, before[number]
        )
        for flip in (1, 0):
            sums.append(along_rows(sketches[flip], -shift, flip))
    kerns = [kerns[i] for i in range(8)]
    sketch_out, sketch, packed = call(
        core_body,
        [shape(own, rank), shape(own, rank), shape(everyone, 512)],
        *sums,
        test_matrix,
        targets,
        ridge,
    )
    packed = exchanged(packed, ALL)
    packed = call(summed_body, shape(everyone, 512), packed)
    packed = exchanged(packed, ALL)
    inverse, state, send = call(
        first_body,
        [shape(rank, rank), shape(8, own), shape(column_devices, own)],
        packed,
        sketch,
        targets,
        ridge,
    )
    product = kernel_times(kerns, exchanged(send, COLUMNS))
    image, send = call(
        image_body,
        [shape(8, own), shape(everyone, 384)],
        exchanged(product, ROWS),
        state,
        sketch,
        targets,
        ridge,
    )
    following, send = call(
        second_body,
        [shape(8, own), shape(everyone, own)],
        exchanged(send, ALL),
        state,
        image,
        inverse,
        sketch,
        targets,
        ridge,
    )
    every = exchanged(send, ALL)
    product = call(last_product_body, shape(everyone, 384), *kerns, every, limit=KLIMIT2)
    coefficients, residual = call(
        finish_body,
        [shape(1, own), shape(1, own)],
        exchanged(product, ALL),
        every,
        state,
        following,
        image,
        targets,
        ridge,
    )
    return coefficients.reshape(own), residual.reshape(own), sketch_out


def solution(mesh):
    split = Mesh(mesh.devices.reshape(2, 2, 4, 4, 2), AXES)

    return jax.shard_map(
        local,
        mesh=split,
        in_specs=(P(ALL, None), P(), P(ALL, None), P(ALL), P()),
        out_specs=(P(ALL), P(ALL), P(ALL, None)),
        check_vma=False,
    )
```

```python
import functools

import jax
import jax.numpy as jnp
from jax import lax
from jax.experimental import pallas as pl
from jax.experimental.pallas import tpu as pltpu
from jax.sharding import Mesh
from jax.sharding import PartitionSpec as P


AXES = ("row_0", "row_1", "row_2", "col_0", "col_1")
ALL = ("col_0", "col_1", "row_0", "row_1", "row_2")
NEAR_COLUMNS = ("row_0", "row_2")
ROWS = ("row_1", "col_0")
LOG2E = 1.4426950408889634
MIB = 1024 * 1024
WIDTH = 16
F32 = jnp.float32
BF16 = jnp.bfloat16
HIGH = lax.Precision.HIGHEST
KERN_SPACE = pltpu.VMEM
ORDER = (2, 1, 3, 0)
KLIMIT = 4
KLIMIT2 = 4


def call(body, outs, *args, scratch=(), limit=4):
    return pl.pallas_call(
        body,
        out_shape=outs,
        scratch_shapes=list(scratch),
        compiler_params=pltpu.CompilerParams(vmem_limit_bytes=limit * MIB),
    )(*args)


def shape(*dims, dtype=F32):
    return jax.ShapeDtypeStruct(dims, dtype)


def exchanged(pieces, axes):
    return lax.all_to_all(pieces, axes, 0, 0, tiled=True)


def split3(value):
    first = value.astype(BF16)
    rest = value - first.astype(F32)
    second = rest.astype(BF16)
    third = (rest - second.astype(F32)).astype(BF16)
    return first, second, third


def parts_body(
    points_ref, scale_ref, test_ref, out_ref, copies_ref, points_scr, scale_scr, message_scr, in_sem, out_sem
):
    inputs = (
        (points_ref, points_scr),
        (scale_ref, scale_scr),
        (test_ref, message_scr.at[:, 128:384]),
    )
    loads = [pltpu.make_async_copy(*pair, in_sem.at[i]) for i, pair in enumerate(inputs)]
    for load in loads:
        load.start()
    loads[0].wait()
    loads[1].wait()
    y = points_scr[...].T * (scale_scr[...] * LOG2E**0.5)
    first = y.astype(BF16).astype(F32)
    second = (y - first).astype(BF16).astype(F32)
    parts = jnp.concatenate([first, second], axis=1).astype(BF16)
    out_ref[...] = parts
    message_scr[:, 0:128] = parts
    loads[2].wait()
    stores = [
        pltpu.make_async_copy(message_scr, copies_ref.at[i], out_sem.at[i])
        for i in range(copies_ref.shape[0])
    ]
    for store in stores:
        store.start()
    for store in stores:
        store.wait()


def parts_and_copies(points, scale, test, copies):
    own, features = points.shape
    lanes = 128 + test.shape[1]
    anywhere = pl.BlockSpec(memory_space=pltpu.HBM)
    return pl.pallas_call(
        parts_body,
        in_specs=[anywhere] * 3,
        out_specs=[pl.BlockSpec(memory_space=pltpu.VMEM), anywhere],
        out_shape=[shape(own, 128, dtype=BF16), pltpu.HBM((copies, own, lanes), BF16)],
        scratch_shapes=[
            pltpu.VMEM((features, own), F32),
            pltpu.VMEM((1, features), F32),
            pltpu.VMEM((own, lanes), BF16),
            pltpu.SemaphoreType.DMA((3,)),
            pltpu.SemaphoreType.DMA((copies,)),
        ],
        compiler_params=pltpu.CompilerParams(vmem_limit_bytes=4 * MIB),
        name="parts",
    )(*(pltpu.with_memory_space_constraint(a, pltpu.HBM) for a in (points.T, scale, test)))


def norms_body(message_ref, norm_ref):
    lane = lax.broadcasted_iota(jnp.int32, (128, 128), 1)
    sub = lax.broadcasted_iota(jnp.int32, (128, 128), 0)
    twice = jnp.where((lane - sub) % 64 == 0, 1.0, 0.0).astype(BF16)
    points = jnp.dot(message_ref[:, 0:128], twice, preferred_element_type=F32)
    squares = -0.25 * (points * points)
    lane8, sub8 = lane[0:8], sub[0:8]
    for base in range(0, message_ref.shape[0], 128):
        packed = jnp.zeros((8, 128), F32)
        for at in range(0, 128, 8):
            total = jnp.sum(squares[base + at : base + at + 8], axis=1, keepdims=True)
            packed = packed + jnp.where(lane8 == sub8 + at, total, 0.0)
        norm_ref[:, base : base + 128] = eight(jnp.sum(packed, axis=0, keepdims=True))


def block_body(*refs, chunk, has_before):
    first_ref, second_ref, message_ref, norm_ref, *rest = refs
    parts = jnp.concatenate([first_ref[...], second_ref[...]], axis=0)
    turned = pltpu.roll(parts.astype(F32), 64, 1)
    points = parts.astype(F32) + turned
    left_norm = -0.25 * jnp.sum(points * points, axis=1, keepdims=True)
    left = jnp.concatenate([parts, turned.astype(BF16)], axis=1)
    total = None
    if has_before:
        own_before_ref, other_before_ref, *rest = rest
        total = jnp.concatenate([own_before_ref[...], other_before_ref[...]], axis=0)
    kern_ref, own_ref, other_ref = rest
    for start in range(0, message_ref.shape[0], chunk):
        span = slice(start, start + chunk)
        right = message_ref[span, 0:128]
        exponent = lax.dot_general(
            left,
            jnp.concatenate([right, right], axis=1),
            (((1,), (1,)), ((), ())),
            preferred_element_type=F32,
        )
        weights = jnp.exp2(exponent + left_norm + norm_ref[0:1, span])
        kern_ref[:, span] = weights
        part = jnp.dot(
            weights.astype(BF16), message_ref[span, 128:], preferred_element_type=F32
        )
        total = part if total is None else total + part
    half = total.shape[0] // 2
    own_ref[...] = total[:half]
    other_ref[...] = total[half:]


def kernel_block(first, second, message, norm, before=()):
    rows, columns, rank = first.shape[0], message.shape[0], message.shape[1] - 128
    return call(
        functools.partial(block_body, chunk=512, has_before=bool(before)),
        [KERN_SPACE((2 * rows, columns), F32), shape(rows, rank), shape(rows, rank)],
        first,
        second,
        message,
        norm,
        *before,
        limit=KLIMIT,
    )


def core_body(
    *refs
):
    *part_refs, test_ref, targets_ref, ridge_ref, sketch_ref, copy_ref, out_ref = refs
    sketch = part_refs[0][...]
    for part_ref in part_refs[1:]:
        sketch = sketch + part_ref[...]
    sketch_ref[...] = sketch
    copy_ref[...] = sketch
    shifted = ridge_ref[0, 0] * test_ref[...].astype(F32) + sketch
    core = lax.dot_general(
        shifted, sketch, (((0,), (0,)), ((), ())), precision=HIGH, preferred_element_type=F32
    )
    targets = jnp.broadcast_to(targets_ref[...], (8, 256))
    projected = jnp.dot(targets, sketch, precision=HIGH, preferred_element_type=F32)
    square = jnp.sum(targets[0:1] * targets[0:1], axis=1, keepdims=True)
    row = lax.broadcasted_iota(jnp.int32, (8, 128), 0)
    extra = jnp.where(row == 2, square, 0.0)
    extra = jnp.where(row == 1, projected[:, 128:256], extra)
    extra = jnp.where(row == 0, projected[:, 0:128], extra)
    out_ref[:, 0:256] = core[0:128]
    out_ref[:, 256:384] = core[128:256, 128:256]
    out_ref[:, 384:512] = jnp.zeros((128, 128), F32)
    out_ref[0:8, 384:512] = extra


def summed_body(parts_ref, out_ref):
    out_ref[...] = jnp.broadcast_to(jnp.sum(parts_ref[...], axis=0, keepdims=True), out_ref.shape)


def inverted(work_ref):
    size = work_ref.shape[0]
    panels = size // WIDTH
    per_window = 128 // WIDTH
    sub = lax.broadcasted_iota(jnp.int32, (WIDTH, 1), 0)
    lanes = lax.broadcasted_iota(jnp.int32, (1, size), 1)

    def column(block, step, j):
        index = jnp.full((WIDTH, 128), 0, jnp.int32) + ((step % per_window) * WIDTH + j)
        window = jnp.where(step < per_window, block[:, 0:128], block[:, 128:256])
        return jnp.take_along_axis(window, index, axis=1)

    def wide(value):
        return jnp.concatenate([value, value], axis=1)

    def eliminated(panel, step):
        diag = [column(panel, step, j) for j in range(WIDTH)]
        for j in range(0, WIDTH, 2):
            a, b = diag[j][j : j + 1, :], diag[j + 1][j : j + 1, :]
            c, d = diag[j][j + 1 : j + 2, :], diag[j + 1][j + 1 : j + 2, :]
            inverse = 1.0 / (a * d - b * c)
            upper, lower = sub == j, sub == j + 1

            def swept(block, first, second, spread=lambda value: value):
                top, bottom = block[j : j + 1, :], block[j + 1 : j + 2, :]
                new_top = (spread(d) * top - spread(b) * bottom) * spread(inverse)
                new_bottom = (spread(a) * bottom - spread(c) * top) * spread(inverse)
                rest = block - first * new_top - second * new_bottom
                return jnp.where(upper, new_top, jnp.where(lower, new_bottom, rest))

            for k in range(j + 2, WIDTH):
                diag[k] = swept(diag[k], diag[j], diag[j + 1])
            panel = jnp.where(lanes == step * WIDTH + j, jnp.where(upper, 1.0, 0.0), panel)
            panel = jnp.where(lanes == step * WIDTH + j + 1, jnp.where(lower, 1.0, 0.0), panel)
            panel = swept(panel, wide(diag[j]), wide(diag[j + 1]), wide)
        return panel

    def split(value):
        return [part.astype(F32) for part in split3(value)]

    def stacked(parts):
        return jnp.concatenate(parts, axis=0).astype(BF16)

    def panel_step(step, carry):
        panel, factors = carry
        following = jnp.minimum(step + 1, panels - 1)
        here = pl.ds(pl.multiple_of(step * WIDTH, WIDTH), WIDTH)
        ahead = work_ref[pl.ds(pl.multiple_of(following * WIDTH, WIDTH), WIDTH), :]
        inside = (lanes >= step * WIDTH) & (lanes < step * WIDTH + WIDTH)
        following_rows = jnp.where(inside, 0.0, ahead)
        for j in range(WIDTH):
            following_rows = following_rows - wide(column(ahead, step, j)) * panel[j : j + 1, :]
        f1, f2, f3 = split(factors)
        p1, p2, p3 = split(panel)
        update = lax.dot_general(
            stacked([f1, f1, f2, f2, f1, f3]),
            stacked([p1, p2, p1, p2, p3, p1]),
            (((0,), (0,)), ((), ())),
            preferred_element_type=F32,
        )
        work_ref[...] = jnp.where(inside, 0.0, work_ref[...]) - update
        work_ref[here, :] = panel
        following_factors = jnp.where(lanes < following * WIDTH, -following_rows, following_rows)
        return eliminated(following_rows, following), following_factors

    start = work_ref[0:WIDTH, :]
    lax.fori_loop(0, panels, panel_step, (eliminated(start, 0), start))


def eight(row):
    return jnp.broadcast_to(row, (8, row.shape[1]))


def row_dot(a, b):
    return jnp.sum(a * b, axis=1, keepdims=True)


def times(vector, matrix, transposed=False):
    dims = (((1,), (1 if transposed else 0,)), ((), ()))
    return lax.dot_general(vector, matrix, dims, precision=HIGH, preferred_element_type=F32)


def first_body(packed_ref, sketch_ref, targets_ref, ridge_ref, inverse_ref, state_ref, send_ref):
    inverse_ref[0:128, :] = packed_ref[:, 0:256]
    inverse_ref[128:256, 0:128] = packed_ref[:, 128:256].T
    inverse_ref[128:256, 128:256] = packed_ref[:, 256:384]
    inverted(inverse_ref)
    projected = jnp.concatenate([packed_ref[0:1, 384:512], packed_ref[1:2, 384:512]], axis=1)
    square = packed_ref[2:3, 384:385]
    solved = times(eight(projected), inverse_ref[...])
    fitted = times(solved, sketch_ref[...], transposed=True)
    ridge = ridge_ref[0, 0]
    direction = (targets_ref[...] - fitted[0:1]) / ridge
    descent = (square - row_dot(projected, solved[0:1])) / ridge
    state_ref[0:1, :] = direction
    state_ref[1:2, :] = projected
    state_ref[2:3, :] = jnp.broadcast_to(square, (1, 256))
    state_ref[3:4, :] = jnp.broadcast_to(descent, (1, 256))
    send_ref[...] = jnp.broadcast_to(direction, send_ref.shape)


def products(kern_refs, vector):
    sub = lax.broadcasted_iota(jnp.int32, (8, 128), 0)
    lane = lax.broadcasted_iota(jnp.int32, (8, 128), 1)
    chips = len(ORDER)
    tiles = kern_refs[0].shape[1] // 128
    for number, shift in enumerate(ORDER):
        pair = (kern_refs[number], kern_refs[number + chips])
        for half in range(2):
            pieces = []
            for flip in range(2):
                packed = jnp.zeros((8, 128), F32)
                for start in range(0, 128, 64):
                    base = flip * 256 + half * 128 + start
                    acc = [None] * 8
                    for k in range(2 * tiles):
                        span = slice(k % 2 * 128, k % 2 * 128 + 128)
                        piece = eight(vector[k // 2 : k // 2 + 1, span])
                        at = k % tiles * 128
                        for g in range(8):
                            block = pair[k // tiles][
                                base + g * 8 : base + g * 8 + 8, at : at + 128
                            ]
                            acc[g] = block * piece if k == 0 else acc[g] + block * piece
                    for g in range(8):
                        total = jnp.sum(acc[g], axis=1, keepdims=True)
                        packed = packed + jnp.where(lane == sub + (start + g * 8), total, 0.0)
                pieces.append(jnp.sum(packed, axis=0, keepdims=True))
            yield shift, half, pieces


def own_first(lower, upper):
    core = lax.axis_index("col_1")
    return jnp.concatenate(
        [jnp.where(core == 0, lower, upper), jnp.where(core == 0, upper, lower)], axis=0
    )


def owner(shift):
    chips = len(ORDER)
    return (lax.axis_index("col_0") + (chips - shift)) % chips


def product_body(*refs):
    *kern_refs, vector_ref, partner_ref, out_ref = refs
    half_y = lax.axis_index("row_1")
    chips = len(ORDER)
    vector = jnp.concatenate([vector_ref[...], partner_ref[...]], axis=0)
    for shift, half, pieces in products(kern_refs, vector):
        span = slice(half * 128, half * 128 + 128)
        out_ref[half_y * chips + owner(shift), :, span] = eight(pieces[0])
        out_ref[(1 - half_y) * chips + owner(shift), :, span] = eight(pieces[1])


def last_product_body(*refs):
    *kern_refs, vector_ref, out_ref = refs
    chip, core = lax.axis_index("col_0"), lax.axis_index("col_1")
    far_y, half_y, z = lax.axis_index("row_0"), lax.axis_index("row_1"), lax.axis_index("row_2")

    def group(chip, core, far_y):
        return pl.ds(pl.multiple_of(chip * 32 + core * 16 + far_y * 8, 8), 8)

    def columns_of(core):
        rows = [vector_ref[group(chip, core, far), :] for far in range(2)]
        return jnp.concatenate(
            [jnp.where(half_y == 0, block[0:4], block[4:8]) for block in rows], axis=0
        )

    sub = lax.broadcasted_iota(jnp.int32, (8, 128), 0)
    mine = sub // 4 == half_y
    curve = jnp.zeros((8, 128), F32)
    out_ref[...] = jnp.zeros(out_ref.shape, F32)
    vector = own_first(columns_of(0), columns_of(1))
    for shift, half, pieces in products(kern_refs, vector):
        span = slice(half * 128, half * 128 + 128)
        rows = group(owner(shift), core, far_y)
        both = jnp.where(mine, pieces[0], pieces[1])
        out_ref[rows, span] = both
        curve = curve + jnp.where(sub % 4 == z, both * vector_ref[rows, span], 0.0)
    curve = jnp.sum(curve, axis=0, keepdims=True)
    out_ref[:, 256:384] = jnp.broadcast_to(curve, (out_ref.shape[0], 128))


def kernel_times(kerns, vector):
    partner = lax.ppermute(vector, "col_1", [(0, 1), (1, 0)])
    return call(product_body, shape(8, 8, 256), *kerns, vector, partner, limit=KLIMIT2)


def image_body(parts_ref, state_ref, sketch_ref, targets_ref, ridge_ref, image_ref, send_ref):
    image = jnp.sum(parts_ref[...], axis=0)[0:1] + ridge_ref[0, 0] * state_ref[0:1, :]
    image_ref[...] = eight(image)
    along = times(eight(image), sketch_ref[...])[0:1]
    lane = lax.broadcasted_iota(jnp.int32, (1, 128), 1)
    sums = jnp.where(
        lane == 0,
        row_dot(state_ref[0:1, :], image),
        jnp.where(
            lane == 1, row_dot(image, image), jnp.where(lane == 2, row_dot(targets_ref[...], image), 0.0)
        ),
    )
    send_ref[:, 0:256] = jnp.broadcast_to(along, (send_ref.shape[0], 256))
    send_ref[:, 256:384] = jnp.broadcast_to(sums, (send_ref.shape[0], 128))


def second_body(
    parts_ref, state_ref, image_ref, inverse_ref, sketch_ref, targets_ref, ridge_ref, next_ref, send_ref
):
    sums = jnp.sum(parts_ref[...], axis=0, keepdims=True)
    along = sums[:, 0:256]
    curve, image_square, cross = sums[:, 256:257], sums[:, 257:258], sums[:, 258:259]
    ridge = ridge_ref[0, 0]
    descent = state_ref[3:4, :]
    step = descent / curve
    projected = state_ref[1:2, :] - step * along
    solved = times(eight(projected), inverse_ref[...])
    fitted = times(solved, sketch_ref[...], transposed=True)[0:1]
    resid = targets_ref[...] - step * image_ref[0:1, :]
    square = state_ref[2:3, :] - 2.0 * step * cross + step * step * image_square
    fresh = (square - row_dot(projected, solved[0:1])) / ridge
    direction = (resid - fitted) / ridge + fresh / descent * state_ref[0:1, :]
    next_ref[0:1, :] = direction
    next_ref[1:2, :] = step
    next_ref[2:3, :] = fresh
    send_ref[...] = jnp.broadcast_to(direction, send_ref.shape)


def finish_body(
    parts_ref,
    every_ref,
    state_ref,
    next_ref,
    image_ref,
    targets_ref,
    ridge_ref,
    coefficients_ref,
    residual_ref,
):
    ridge = ridge_ref[0, 0]
    group = lax.axis_index("col_1") * 2 + lax.axis_index("row_0")
    direction = next_ref[0:1, :]
    row = lax.broadcasted_iota(jnp.int32, (parts_ref.shape[0], 256), 0)
    mine = (row % 32 // 8 == group) & (row % 4 == lax.axis_index("row_2"))
    last = jnp.sum(jnp.where(mine, parts_ref[:, 0:256], 0.0), axis=0, keepdims=True)
    last = last + ridge * direction
    every = every_ref[...]
    square = jnp.sum(jnp.sum(every * every, axis=0, keepdims=True), axis=1, keepdims=True)
    curve = jnp.sum(
        jnp.sum(parts_ref[:, 256:384], axis=0, keepdims=True), axis=1, keepdims=True
    )
    step = next_ref[1:2, :]
    last_step = next_ref[2:3, :] / (curve + ridge * square)
    coefficients_ref[...] = step * state_ref[0:1, :] + last_step * direction
    residual_ref[...] = targets_ref[...] - step * image_ref[0:1, :] - last_step * last


def local(points, feature_scale, test_matrix, targets, ridge):
    everyone = lax.axis_size(ALL)
    near_devices = lax.axis_size(NEAR_COLUMNS)
    own, rank = test_matrix.shape
    ridge = ridge.reshape(1, 1)
    targets = targets.reshape(1, own)
    scale = feature_scale.reshape(1, -1)
    parts, copies = parts_and_copies(points, scale, test_matrix, near_devices)
    chips = lax.axis_size("col_0")

    def along_rows(value, shift, flip):
        pairs = [
            (i, (i // chips ^ flip) * chips + (i + shift) % chips) for i in range(2 * chips)
        ]
        return lax.ppermute(value, ROWS, pairs) if shift or flip else value

    chunks = {
        (shift, flip): along_rows(parts, shift, flip) for shift in ORDER for flip in (0, 1)
    }
    message = exchanged(copies, NEAR_COLUMNS).reshape(-1, 128 + rank)
    message, chunks = lax.optimization_barrier((message, chunks))
    partner = lax.ppermute(message, "col_1", [(0, 1), (1, 0)])
    norm = call(norms_body, shape(8, message.shape[0]), message)
    kerns, before, sums = {}, {}, []

    def near_block(number):
        shift = ORDER[number]
        kerns[number], *before[number] = kernel_block(
            chunks[shift, 0], chunks[shift, 1], message, norm
        )

    for number in range(3):
        near_block(number)
    other_norm = call(norms_body, shape(8, message.shape[0]), partner)
    for number, shift in enumerate(ORDER):
        if number == 3:
            near_block(number)
        kerns[number + 4], *sketches = kernel_block(
            chunks[shift, 0], chunks[shift, 1], partner, other_norm, before[number]
        )
        for flip in (1, 0):
            sums.append(along_rows(sketches[flip], -shift, flip))
    kerns = [kerns[i] for i in range(8)]
    sketch_out, sketch, packed = call(
        core_body,
        [shape(own, rank), shape(own, rank), shape(everyone, 512)],
        *sums,
        test_matrix,
        targets,
        ridge,
    )
    packed = exchanged(packed, ALL)
    packed = call(summed_body, shape(everyone, 512), packed)
    packed = exchanged(packed, ALL)
    inverse, state, send = call(
        first_body,
        [shape(rank, rank), shape(8, own), shape(near_devices, own)],
        packed,
        sketch,
        targets,
        ridge,
    )
    product = kernel_times(kerns, exchanged(send, NEAR_COLUMNS))
    image, send = call(
        image_body,
        [shape(8, own), shape(everyone, 384)],
        exchanged(product, ROWS),
        state,
        sketch,
        targets,
        ridge,
    )
    following, send = call(
        second_body,
        [shape(8, own), shape(everyone, own)],
        exchanged(send, ALL),
        state,
        image,
        inverse,
        sketch,
        targets,
        ridge,
    )
    every = exchanged(send, ALL)
    product = call(last_product_body, shape(everyone, 384), *kerns, every, limit=KLIMIT2)
    coefficients, residual = call(
        finish_body,
        [shape(1, own), shape(1, own)],
        exchanged(product, ALL),
        every,
        state,
        following,
        image,
        targets,
        ridge,
    )
    return coefficients.reshape(own), residual.reshape(own), sketch_out


def solution(mesh):
    split = Mesh(mesh.devices.reshape(2, 2, 4, 4, 2), AXES)

    return jax.shard_map(
        local,
        mesh=split,
        in_specs=(P(ALL, None), P(), P(ALL, None), P(ALL), P()),
        out_specs=(P(ALL), P(ALL), P(ALL, None)),
        check_vma=False,
    )
```

```python
import functools

import jax
import jax.numpy as jnp
from jax import lax
from jax.experimental import pallas as pl
from jax.experimental.pallas import tpu as pltpu
from jax.sharding import Mesh
from jax.sharding import PartitionSpec as P


AXES = ("row_0", "row_1", "row_2", "col_0", "col_1")
ALL = ("col_0", "col_1", "row_0", "row_1", "row_2")
NEAR_COLUMNS = ("row_0", "row_2")
COLUMNS = ("col_1", "row_0", "row_2")
ROWS = ("row_1", "col_0")
LOG2E = 1.4426950408889634
MIB = 1024 * 1024
WIDTH = 16
F32 = jnp.float32
BF16 = jnp.bfloat16
HIGH = lax.Precision.HIGHEST
KERN_SPACE = pltpu.VMEM
ORDER = (1, 3, 2, 0)
KLIMIT = 4
KLIMIT2 = 4


def call(body, outs, *args, scratch=(), limit=4):
    return pl.pallas_call(
        body,
        out_shape=outs,
        scratch_shapes=list(scratch),
        compiler_params=pltpu.CompilerParams(vmem_limit_bytes=limit * MIB),
    )(*args)


def shape(*dims, dtype=F32):
    return jax.ShapeDtypeStruct(dims, dtype)


def exchanged(pieces, axes):
    return lax.all_to_all(pieces, axes, 0, 0, tiled=True)


def split3(value):
    first = value.astype(BF16)
    rest = value - first.astype(F32)
    second = rest.astype(BF16)
    third = (rest - second.astype(F32)).astype(BF16)
    return first, second, third


def parts_body(
    points_ref, scale_ref, test_ref, out_ref, copies_ref, points_scr, scale_scr, message_scr, in_sem, out_sem
):
    inputs = (
        (points_ref, points_scr),
        (scale_ref, scale_scr),
        (test_ref, message_scr.at[:, 128:384]),
    )
    loads = [pltpu.make_async_copy(*pair, in_sem.at[i]) for i, pair in enumerate(inputs)]
    for load in loads:
        load.start()
    loads[0].wait()
    loads[1].wait()
    y = points_scr[...].T * (scale_scr[...] * LOG2E**0.5)
    first = y.astype(BF16).astype(F32)
    second = (y - first).astype(BF16).astype(F32)
    parts = jnp.concatenate([first, second], axis=1).astype(BF16)
    out_ref[...] = parts
    message_scr[:, 0:128] = parts
    loads[2].wait()
    stores = [
        pltpu.make_async_copy(message_scr, copies_ref.at[i], out_sem.at[i])
        for i in range(copies_ref.shape[0])
    ]
    for store in stores:
        store.start()
    for store in stores:
        store.wait()


def parts_and_copies(points, scale, test, copies):
    own, features = points.shape
    lanes = 128 + test.shape[1]
    anywhere = pl.BlockSpec(memory_space=pltpu.HBM)
    return pl.pallas_call(
        parts_body,
        in_specs=[anywhere] * 3,
        out_specs=[pl.BlockSpec(memory_space=pltpu.VMEM), anywhere],
        out_shape=[shape(own, 128, dtype=BF16), pltpu.HBM((copies, own, lanes), BF16)],
        scratch_shapes=[
            pltpu.VMEM((features, own), F32),
            pltpu.VMEM((1, features), F32),
            pltpu.VMEM((own, lanes), BF16),
            pltpu.SemaphoreType.DMA((3,)),
            pltpu.SemaphoreType.DMA((copies,)),
        ],
        compiler_params=pltpu.CompilerParams(vmem_limit_bytes=4 * MIB),
        name="parts",
    )(*(pltpu.with_memory_space_constraint(a, pltpu.HBM) for a in (points.T, scale, test)))


def norms_body(message_ref, norm_ref):
    lane = lax.broadcasted_iota(jnp.int32, (128, 128), 1)
    sub = lax.broadcasted_iota(jnp.int32, (128, 128), 0)
    twice = jnp.where((lane - sub) % 64 == 0, 1.0, 0.0).astype(BF16)
    points = jnp.dot(message_ref[:, 0:128], twice, preferred_element_type=F32)
    squares = -0.25 * (points * points)
    lane8, sub8 = lane[0:8], sub[0:8]
    for base in range(0, message_ref.shape[0], 128):
        packed = jnp.zeros((8, 128), F32)
        for at in range(0, 128, 8):
            total = jnp.sum(squares[base + at : base + at + 8], axis=1, keepdims=True)
            packed = packed + jnp.where(lane8 == sub8 + at, total, 0.0)
        norm_ref[:, base : base + 128] = eight(jnp.sum(packed, axis=0, keepdims=True))


def block_body(*refs, chunk, has_before):
    first_ref, second_ref, message_ref, norm_ref, *rest = refs
    parts = jnp.concatenate([first_ref[...], second_ref[...]], axis=0)
    turned = pltpu.roll(parts.astype(F32), 64, 1)
    points = parts.astype(F32) + turned
    left_norm = -0.25 * jnp.sum(points * points, axis=1, keepdims=True)
    left = jnp.concatenate([parts, turned.astype(BF16)], axis=1)
    total = None
    if has_before:
        own_before_ref, other_before_ref, *rest = rest
        total = jnp.concatenate([own_before_ref[...], other_before_ref[...]], axis=0)
    kern_ref, own_ref, other_ref = rest
    for start in range(0, message_ref.shape[0], chunk):
        span = slice(start, start + chunk)
        right = message_ref[span, 0:128]
        exponent = lax.dot_general(
            left,
            jnp.concatenate([right, right], axis=1),
            (((1,), (1,)), ((), ())),
            preferred_element_type=F32,
        )
        weights = jnp.exp2(exponent + left_norm + norm_ref[0:1, span])
        kern_ref[:, span] = weights
        part = jnp.dot(
            weights.astype(BF16), message_ref[span, 128:], preferred_element_type=F32
        )
        total = part if total is None else total + part
    half = total.shape[0] // 2
    own_ref[...] = total[:half]
    other_ref[...] = total[half:]


def kernel_block(first, second, message, norm, before=()):
    rows, columns, rank = first.shape[0], message.shape[0], message.shape[1] - 128
    return call(
        functools.partial(block_body, chunk=512, has_before=bool(before)),
        [KERN_SPACE((2 * rows, columns), F32), shape(rows, rank), shape(rows, rank)],
        first,
        second,
        message,
        norm,
        *before,
        limit=KLIMIT,
    )


def core_body(
    *refs
):
    *part_refs, test_ref, targets_ref, ridge_ref, sketch_ref, copy_ref, out_ref = refs
    sketch = part_refs[0][...]
    for part_ref in part_refs[1:]:
        sketch = sketch + part_ref[...]
    sketch_ref[...] = sketch
    copy_ref[...] = sketch
    shifted = ridge_ref[0, 0] * test_ref[...].astype(F32) + sketch
    core = lax.dot_general(
        shifted, sketch, (((0,), (0,)), ((), ())), precision=HIGH, preferred_element_type=F32
    )
    targets = jnp.broadcast_to(targets_ref[...], (8, 256))
    projected = jnp.dot(targets, sketch, precision=HIGH, preferred_element_type=F32)
    square = jnp.sum(targets[0:1] * targets[0:1], axis=1, keepdims=True)
    row = lax.broadcasted_iota(jnp.int32, (8, 128), 0)
    extra = jnp.where(row == 2, square, 0.0)
    extra = jnp.where(row == 1, projected[:, 128:256], extra)
    extra = jnp.where(row == 0, projected[:, 0:128], extra)
    out_ref[:, 0:256] = core[0:128]
    out_ref[:, 256:384] = core[128:256, 128:256]
    out_ref[:, 384:512] = jnp.zeros((128, 128), F32)
    out_ref[0:8, 384:512] = extra


def summed_body(parts_ref, out_ref):
    out_ref[...] = jnp.broadcast_to(jnp.sum(parts_ref[...], axis=0, keepdims=True), out_ref.shape)


def inverted(work_ref):
    size = work_ref.shape[0]
    panels = size // WIDTH
    per_window = 128 // WIDTH
    sub = lax.broadcasted_iota(jnp.int32, (WIDTH, 1), 0)
    lanes = lax.broadcasted_iota(jnp.int32, (1, size), 1)

    def column(block, step, j):
        index = jnp.full((WIDTH, 128), 0, jnp.int32) + ((step % per_window) * WIDTH + j)
        window = jnp.where(step < per_window, block[:, 0:128], block[:, 128:256])
        return jnp.take_along_axis(window, index, axis=1)

    def wide(value):
        return jnp.concatenate([value, value], axis=1)

    def eliminated(panel, step):
        diag = [column(panel, step, j) for j in range(WIDTH)]
        for j in range(0, WIDTH, 2):
            a, b = diag[j][j : j + 1, :], diag[j + 1][j : j + 1, :]
            c, d = diag[j][j + 1 : j + 2, :], diag[j + 1][j + 1 : j + 2, :]
            inverse = 1.0 / (a * d - b * c)
            upper, lower = sub == j, sub == j + 1

            def swept(block, first, second, spread=lambda value: value):
                top, bottom = block[j : j + 1, :], block[j + 1 : j + 2, :]
                new_top = (spread(d) * top - spread(b) * bottom) * spread(inverse)
                new_bottom = (spread(a) * bottom - spread(c) * top) * spread(inverse)
                rest = block - first * new_top - second * new_bottom
                return jnp.where(upper, new_top, jnp.where(lower, new_bottom, rest))

            for k in range(j + 2, WIDTH):
                diag[k] = swept(diag[k], diag[j], diag[j + 1])
            panel = jnp.where(lanes == step * WIDTH + j, jnp.where(upper, 1.0, 0.0), panel)
            panel = jnp.where(lanes == step * WIDTH + j + 1, jnp.where(lower, 1.0, 0.0), panel)
            panel = swept(panel, wide(diag[j]), wide(diag[j + 1]), wide)
        return panel

    def split(value):
        return [part.astype(F32) for part in split3(value)]

    def stacked(parts):
        return jnp.concatenate(parts, axis=0).astype(BF16)

    def panel_step(step, carry):
        panel, factors = carry
        following = jnp.minimum(step + 1, panels - 1)
        here = pl.ds(pl.multiple_of(step * WIDTH, WIDTH), WIDTH)
        ahead = work_ref[pl.ds(pl.multiple_of(following * WIDTH, WIDTH), WIDTH), :]
        inside = (lanes >= step * WIDTH) & (lanes < step * WIDTH + WIDTH)
        following_rows = jnp.where(inside, 0.0, ahead)
        for j in range(WIDTH):
            following_rows = following_rows - wide(column(ahead, step, j)) * panel[j : j + 1, :]
        f1, f2, f3 = split(factors)
        p1, p2, p3 = split(panel)
        update = lax.dot_general(
            stacked([f1, f1, f2, f2, f1, f3]),
            stacked([p1, p2, p1, p2, p3, p1]),
            (((0,), (0,)), ((), ())),
            preferred_element_type=F32,
        )
        work_ref[...] = jnp.where(inside, 0.0, work_ref[...]) - update
        work_ref[here, :] = panel
        following_factors = jnp.where(lanes < following * WIDTH, -following_rows, following_rows)
        return eliminated(following_rows, following), following_factors

    start = work_ref[0:WIDTH, :]
    lax.fori_loop(0, panels, panel_step, (eliminated(start, 0), start))


def eight(row):
    return jnp.broadcast_to(row, (8, row.shape[1]))


def row_dot(a, b):
    return jnp.sum(a * b, axis=1, keepdims=True)


def times(vector, matrix, transposed=False):
    dims = (((1,), (1 if transposed else 0,)), ((), ()))
    return lax.dot_general(vector, matrix, dims, precision=HIGH, preferred_element_type=F32)


def first_body(packed_ref, sketch_ref, targets_ref, ridge_ref, inverse_ref, state_ref, send_ref):
    inverse_ref[0:128, :] = packed_ref[:, 0:256]
    inverse_ref[128:256, 0:128] = packed_ref[:, 128:256].T
    inverse_ref[128:256, 128:256] = packed_ref[:, 256:384]
    inverted(inverse_ref)
    projected = jnp.concatenate([packed_ref[0:1, 384:512], packed_ref[1:2, 384:512]], axis=1)
    square = packed_ref[2:3, 384:385]
    solved = times(eight(projected), inverse_ref[...])
    fitted = times(solved, sketch_ref[...], transposed=True)
    ridge = ridge_ref[0, 0]
    direction = (targets_ref[...] - fitted[0:1]) / ridge
    descent = (square - row_dot(projected, solved[0:1])) / ridge
    state_ref[0:1, :] = direction
    state_ref[1:2, :] = projected
    state_ref[2:3, :] = jnp.broadcast_to(square, (1, 256))
    state_ref[3:4, :] = jnp.broadcast_to(descent, (1, 256))
    send_ref[...] = jnp.broadcast_to(direction, send_ref.shape)


def products(kern_refs, vector):
    sub = lax.broadcasted_iota(jnp.int32, (8, 128), 0)
    lane = lax.broadcasted_iota(jnp.int32, (8, 128), 1)
    chips = len(ORDER)
    tiles = kern_refs[0].shape[1] // 128
    for number, shift in enumerate(ORDER):
        pair = (kern_refs[number], kern_refs[number + chips])
        for half in range(2):
            pieces = []
            for flip in range(2):
                packed = jnp.zeros((8, 128), F32)
                for start in range(0, 128, 64):
                    base = flip * 256 + half * 128 + start
                    acc = [None] * 8
                    for k in range(2 * tiles):
                        span = slice(k % 2 * 128, k % 2 * 128 + 128)
                        piece = eight(vector[k // 2 : k // 2 + 1, span])
                        at = k % tiles * 128
                        for g in range(8):
                            block = pair[k // tiles][
                                base + g * 8 : base + g * 8 + 8, at : at + 128
                            ]
                            acc[g] = block * piece if k == 0 else acc[g] + block * piece
                    for g in range(8):
                        total = jnp.sum(acc[g], axis=1, keepdims=True)
                        packed = packed + jnp.where(lane == sub + (start + g * 8), total, 0.0)
                pieces.append(jnp.sum(packed, axis=0, keepdims=True))
            yield shift, half, pieces


def own_first(lower, upper):
    core = lax.axis_index("col_1")
    return jnp.concatenate(
        [jnp.where(core == 0, lower, upper), jnp.where(core == 0, upper, lower)], axis=0
    )


def owner(shift):
    chips = len(ORDER)
    return (lax.axis_index("col_0") + (chips - shift)) % chips


def product_body(*refs):
    *kern_refs, vector_ref, out_ref = refs
    half_y = lax.axis_index("row_1")
    chips = len(ORDER)
    vector = own_first(vector_ref[0:8, :], vector_ref[8:16, :])
    for shift, half, pieces in products(kern_refs, vector):
        span = slice(half * 128, half * 128 + 128)
        out_ref[half_y * chips + owner(shift), :, span] = eight(pieces[0])
        out_ref[(1 - half_y) * chips + owner(shift), :, span] = eight(pieces[1])


def last_product_body(*refs):
    *kern_refs, vector_ref, out_ref = refs
    chip, core = lax.axis_index("col_0"), lax.axis_index("col_1")
    far_y, half_y, z = lax.axis_index("row_0"), lax.axis_index("row_1"), lax.axis_index("row_2")

    def group(chip, core, far_y):
        return pl.ds(pl.multiple_of(chip * 32 + core * 16 + far_y * 8, 8), 8)

    def columns_of(core):
        rows = [vector_ref[group(chip, core, far), :] for far in range(2)]
        return jnp.concatenate(
            [jnp.where(half_y == 0, block[0:4], block[4:8]) for block in rows], axis=0
        )

    sub = lax.broadcasted_iota(jnp.int32, (8, 128), 0)
    mine = sub // 4 == half_y
    curve = jnp.zeros((8, 128), F32)
    out_ref[...] = jnp.zeros(out_ref.shape, F32)
    vector = own_first(columns_of(0), columns_of(1))
    for shift, half, pieces in products(kern_refs, vector):
        span = slice(half * 128, half * 128 + 128)
        rows = group(owner(shift), core, far_y)
        both = jnp.where(mine, pieces[0], pieces[1])
        out_ref[rows, span] = both
        curve = curve + jnp.where(sub % 4 == z, both * vector_ref[rows, span], 0.0)
    curve = jnp.sum(curve, axis=0, keepdims=True)
    out_ref[:, 256:384] = jnp.broadcast_to(curve, (out_ref.shape[0], 128))


def kernel_times(kerns, vector):
    return call(product_body, shape(8, 8, 256), *kerns, vector, limit=KLIMIT2)


def image_body(parts_ref, state_ref, sketch_ref, targets_ref, ridge_ref, image_ref, send_ref):
    image = jnp.sum(parts_ref[...], axis=0)[0:1] + ridge_ref[0, 0] * state_ref[0:1, :]
    image_ref[...] = eight(image)
    along = times(eight(image), sketch_ref[...])[0:1]
    lane = lax.broadcasted_iota(jnp.int32, (1, 128), 1)
    sums = jnp.where(
        lane == 0,
        row_dot(state_ref[0:1, :], image),
        jnp.where(
            lane == 1, row_dot(image, image), jnp.where(lane == 2, row_dot(targets_ref[...], image), 0.0)
        ),
    )
    send_ref[:, 0:256] = jnp.broadcast_to(along, (send_ref.shape[0], 256))
    send_ref[:, 256:384] = jnp.broadcast_to(sums, (send_ref.shape[0], 128))


def second_body(
    parts_ref, state_ref, image_ref, inverse_ref, sketch_ref, targets_ref, ridge_ref, next_ref, send_ref
):
    sums = jnp.sum(parts_ref[...], axis=0, keepdims=True)
    along = sums[:, 0:256]
    curve, image_square, cross = sums[:, 256:257], sums[:, 257:258], sums[:, 258:259]
    ridge = ridge_ref[0, 0]
    descent = state_ref[3:4, :]
    step = descent / curve
    projected = state_ref[1:2, :] - step * along
    solved = times(eight(projected), inverse_ref[...])
    fitted = times(solved, sketch_ref[...], transposed=True)[0:1]
    resid = targets_ref[...] - step * image_ref[0:1, :]
    square = state_ref[2:3, :] - 2.0 * step * cross + step * step * image_square
    fresh = (square - row_dot(projected, solved[0:1])) / ridge
    direction = (resid - fitted) / ridge + fresh / descent * state_ref[0:1, :]
    next_ref[0:1, :] = direction
    next_ref[1:2, :] = step
    next_ref[2:3, :] = fresh
    send_ref[...] = jnp.broadcast_to(direction, send_ref.shape)


def finish_body(
    parts_ref,
    every_ref,
    state_ref,
    next_ref,
    image_ref,
    targets_ref,
    ridge_ref,
    coefficients_ref,
    residual_ref,
):
    ridge = ridge_ref[0, 0]
    group = lax.axis_index("col_1") * 2 + lax.axis_index("row_0")
    direction = next_ref[0:1, :]
    row = lax.broadcasted_iota(jnp.int32, (parts_ref.shape[0], 256), 0)
    mine = (row % 32 // 8 == group) & (row % 4 == lax.axis_index("row_2"))
    last = jnp.sum(jnp.where(mine, parts_ref[:, 0:256], 0.0), axis=0, keepdims=True)
    last = last + ridge * direction
    every = every_ref[...]
    square = jnp.sum(jnp.sum(every * every, axis=0, keepdims=True), axis=1, keepdims=True)
    curve = jnp.sum(
        jnp.sum(parts_ref[:, 256:384], axis=0, keepdims=True), axis=1, keepdims=True
    )
    step = next_ref[1:2, :]
    last_step = next_ref[2:3, :] / (curve + ridge * square)
    coefficients_ref[...] = step * state_ref[0:1, :] + last_step * direction
    residual_ref[...] = targets_ref[...] - step * image_ref[0:1, :] - last_step * last


def local(points, feature_scale, test_matrix, targets, ridge):
    everyone = lax.axis_size(ALL)
    column_devices, near_devices = lax.axis_size(COLUMNS), lax.axis_size(NEAR_COLUMNS)
    own, rank = test_matrix.shape
    ridge = ridge.reshape(1, 1)
    targets = targets.reshape(1, own)
    scale = feature_scale.reshape(1, -1)
    parts, copies = parts_and_copies(points, scale, test_matrix, near_devices)
    chips = lax.axis_size("col_0")

    def along_rows(value, shift, flip):
        pairs = [
            (i, (i // chips ^ flip) * chips + (i + shift) % chips) for i in range(2 * chips)
        ]
        return lax.ppermute(value, ROWS, pairs) if shift or flip else value

    chunks = {}
    for shift in ORDER:
        for flip in (0, 1):
            chunks[shift, flip] = along_rows(parts, shift, flip)
    message = exchanged(copies, NEAR_COLUMNS).reshape(-1, 128 + rank)
    early = {key: value for key, value in chunks.items() if key[0] != 2}
    message, early = lax.optimization_barrier((message, early))
    chunks.update(early)
    partner = lax.ppermute(message, "col_1", [(0, 1), (1, 0)])
    norm = call(norms_body, shape(8, message.shape[0]), message)
    kerns, before, sums = {}, {}, []

    def near_block(number):
        shift = ORDER[number]
        kerns[number], *before[number] = kernel_block(
            chunks[shift, 0], chunks[shift, 1], message, norm
        )

    for number in range(3):
        near_block(number)
    other_norm = call(norms_body, shape(8, message.shape[0]), partner)
    for number, shift in enumerate(ORDER):
        if number == 3:
            near_block(number)
        kerns[number + 4], *sketches = kernel_block(
            chunks[shift, 0], chunks[shift, 1], partner, other_norm, before[number]
        )
        for flip in (1, 0):
            sums.append(along_rows(sketches[flip], -shift, flip))
    kerns = [kerns[i] for i in range(8)]
    sketch_out, sketch, packed = call(
        core_body,
        [shape(own, rank), shape(own, rank), shape(everyone, 512)],
        *sums,
        test_matrix,
        targets,
        ridge,
    )
    packed = exchanged(packed, ALL)
    packed = call(summed_body, shape(everyone, 512), packed)
    packed = exchanged(packed, ALL)
    inverse, state, send = call(
        first_body,
        [shape(rank, rank), shape(8, own), shape(column_devices, own)],
        packed,
        sketch,
        targets,
        ridge,
    )
    product = kernel_times(kerns, exchanged(send, COLUMNS))
    image, send = call(
        image_body,
        [shape(8, own), shape(everyone, 384)],
        exchanged(product, ROWS),
        state,
        sketch,
        targets,
        ridge,
    )
    following, send = call(
        second_body,
        [shape(8, own), shape(everyone, own)],
        exchanged(send, ALL),
        state,
        image,
        inverse,
        sketch,
        targets,
        ridge,
    )
    every = exchanged(send, ALL)
    product = call(last_product_body, shape(everyone, 384), *kerns, every, limit=KLIMIT2)
    coefficients, residual = call(
        finish_body,
        [shape(1, own), shape(1, own)],
        exchanged(product, ALL),
        every,
        state,
        following,
        image,
        targets,
        ridge,
    )
    return coefficients.reshape(own), residual.reshape(own), sketch_out


def solution(mesh):
    split = Mesh(mesh.devices.reshape(2, 2, 4, 4, 2), AXES)

    return jax.shard_map(
        local,
        mesh=split,
        in_specs=(P(ALL, None), P(), P(ALL, None), P(ALL), P()),
        out_specs=(P(ALL), P(ALL), P(ALL, None)),
        check_vma=False,
    )
```
